32 devices in a mesh: seq: 8 (over z, x), tp: 4 (over y, core).
Axes of the slice: x: 2, y: 2, z: 4, core: 2. Of those that a mesh axis runs over, the one named last changes fastest.
Arguments:
- queries: bfloat16 [1536, 4096], P('seq', 'tp'), may hold values from -80 to 80
- keys: bfloat16 [1536, 512], P('seq', 'tp'), may hold values from -4 to 4
- values: bfloat16 [1536, 512], P('seq', 'tp'), may hold values from -6 to 6
- segment_ids: int32 [1536], P('seq'), may hold values from 0 to 15, never falling along the last dimension, each value on 1 to 1152 neighbouring positions
- out_weight: bfloat16 [4096, 8192], P('tp', 'seq'), may hold values from -0.09375 to 0.09375
Outputs:
- projected: bfloat16 [1536, 8192], P('seq', 'tp')
The draws below stay inside these ranges and needn't reach their ends.
Inputs may be any that keep to these rules, and one draw needn't show every extreme that they name: `segment_ids`: segment numbers never fall along the sequence and every number from 0 to 15 occurs; no document has more than 1152 tokens and one has exactly that many.
All inputs are finite; a program needn't handle non-finite values.
Results may differ from the reference program's by a relative error of at most 0.012.
Values may be sent and summed in bfloat16 or wider, within the bound.
A program may use at most 128 MiB of HBM per device.

```python
import math
import jax
import jax.numpy as jnp
import numpy as np
from jax import lax

HEADS = 32
KV_HEADS = 4
HEAD_DIM = 128
OUT_WIDTH = 8192
SEGMENTS = 16
TOKENS = 1536
N_TP = 4


def draw_key_field(key):
    base_draw = jax.random.normal(jax.random.fold_in(key, 11), (TOKENS, KV_HEADS * HEAD_DIM), jnp.float32)
    return jnp.clip(base_draw, -4.0, 4.0)


def draw_keys(key, part):
    return draw_key_field(key).astype(jnp.bfloat16)


def draw_queries(key, part):
    fresh_draw = 3.0 * jnp.clip(jax.random.normal(jax.random.fold_in(key, 12), (TOKENS, HEADS * HEAD_DIM), jnp.float32), -6.0, 6.0)
    return fresh_draw.astype(jnp.bfloat16)


def levels(stream_key, dims, pieces, low, top_value):
    level, own = 1.0, jax.random.fold_in(stream_key, 6)
    for dim, parts in pieces:
        heights = jnp.exp(jax.random.uniform(jax.random.fold_in(own, dim), (parts,), jnp.float32, low / len(pieces), top_value / len(pieces)))
        level = level * jnp.repeat(heights, dims[dim] // parts).reshape([-1 if axis == dim else 1 for axis in range(len(dims))])
    return level


def length_profile(amount, total, most, skew):
    loads = [(1 << 20) // math.isqrt(grade ** skew) + 1 for grade in range(2, amount + 1)]
    spare, given = total - most - (amount - 1), [1] * (amount - 1)
    while spare > 0:
        free = [i for i in range(amount - 1) if given[i] < most]
        whole, remaining = sum([loads[i] for i in free]), spare
        for i in free:
            extra = min(most - given[i], max(1, remaining * loads[i] // whole), spare)
            given[i] = given[i] + extra
            spare = spare - extra
    return np.array([most] + given)


def uneven(own_key, amount, total, reach, lean):
    if amount == 2:
        one = jax.random.randint(own_key, (), max(1, total - reach), min(reach, total - 1) + 1)
        return jnp.stack([one, total - one])
    sizes = jnp.asarray(length_profile(amount, total, reach, lean), jnp.int32)
    twos = (amount - 1) // 2
    donor, taker = sizes[1:1 + 2 * twos:2], sizes[2:2 + 2 * twos:2]
    slack = jnp.minimum(donor - 1, reach - taker)
    shifted = jax.random.randint(jax.random.fold_in(own_key, 1), (twos,), 0, 1 << 20) % (slack + 1)
    sizes = sizes.at[1:1 + 2 * twos:2].set(donor - shifted).at[2:2 + 2 * twos:2].set(taker + shifted)
    return sizes[jax.random.permutation(jax.random.fold_in(own_key, 2), amount)]


def centred(stream_key, extent, width, most, split=(), kind=jnp.bfloat16):
    result = jax.random.normal(stream_key, extent, jnp.float32) * width
    if len(split) > 0:
        result = levels(stream_key, extent, split, -0.22, 0.18) * result
    return jnp.clip(result, min=-most, max=most).astype(kind)


def setup_inputs(seed: int = 0) -> dict:
    splits = jax.random.split(jax.random.key(seed), 6)
    return {
        "queries": draw_queries(jax.random.fold_in(splits[5], 71), 0),
        "keys": draw_keys(jax.random.fold_in(splits[5], 71), 0),
        "values": centred(splits[2], (TOKENS, KV_HEADS * HEAD_DIM), 1.0, 6.0, ((0, 8), (1, 4))),
        "segment_ids": jnp.searchsorted(jnp.cumsum(uneven(splits[3], SEGMENTS, TOKENS, 3 * TOKENS // 4, 2)), jnp.arange(TOKENS), side="right").astype(jnp.int32),
        "out_weight": centred(splits[4], (HEADS * HEAD_DIM, OUT_WIDTH), (HEADS * HEAD_DIM) ** -0.5, 0.09375, ((0, 4), (1, 8))),
    }


rope_base = 500000.0
masked_score = -1e+30

def rotate_heads(inputs, positions, head_dim):
    row_count = inputs.shape[0]
    head_count = inputs.shape[1] // head_dim
    half_dim = head_dim // 2
    widened = inputs.astype(jnp.float32).reshape(row_count, head_count, head_dim)
    exponent = jnp.arange(half_dim, dtype=jnp.float32) * (2.0 / head_dim)
    inverse = jnp.power(jnp.float32(rope_base), -exponent)
    angles = positions.astype(jnp.float32)[:, None] * inverse[None, :]
    cosine_table = jnp.cos(angles)[:, None, :]
    sine_table = jnp.sin(angles)[:, None, :]
    first_half = widened[:, :, :half_dim]
    second_half = widened[:, :, half_dim:]
    turned = jnp.concatenate([first_half * cosine_table - second_half * sine_table, second_half * cosine_table + first_half * sine_table], axis=2)
    return turned.reshape(row_count, head_count * head_dim).astype(jnp.bfloat16)

def doc_counts_of(segment_ids, segments):
    labels = jnp.arange(segments, dtype=jnp.int32)
    return lax.optimization_barrier(jnp.sum((segment_ids[None, :] == labels[:, None]).astype(jnp.int32), axis=1))

def first_rows(segment, starts):
    labels = jnp.arange(starts.shape[0], dtype=jnp.int32)
    return lax.optimization_barrier(jnp.sum(jnp.where(segment[:, None] == labels[None, :], starts[None, :], 0), axis=1)).astype(jnp.int32)

def reference(queries, keys, values, segment_ids, out_weight):
    counts = doc_counts_of(segment_ids, SEGMENTS)
    doc_ends = jnp.cumsum(counts).astype(jnp.int32)
    starts = doc_ends - counts
    every_row = jnp.arange(TOKENS, dtype=jnp.int32)
    positions = every_row - first_rows(segment_ids, starts)
    query_rot = rotate_heads(queries, positions, HEAD_DIM)
    key_rot = rotate_heads(keys, positions, HEAD_DIM)
    group_size = HEADS // KV_HEADS
    score_scale = 1.0 / math.sqrt(HEAD_DIM)
    key_full = lax.optimization_barrier(key_rot).astype(jnp.float32).reshape(TOKENS, KV_HEADS, HEAD_DIM)
    value_full = values.astype(jnp.float32).reshape(TOKENS, KV_HEADS, HEAD_DIM)
    query_block = 128 if TOKENS % 128 == 0 else TOKENS

    def attend(block_number):
        first_row = block_number * query_block
        query_tile = lax.dynamic_slice_in_dim(query_rot, first_row, query_block, 0)
        query_tile = lax.optimization_barrier(query_tile).astype(jnp.float32).reshape(query_block, KV_HEADS, group_size, HEAD_DIM)
        query_rows = first_row + jnp.arange(query_block, dtype=jnp.int32)
        query_segs = lax.dynamic_slice_in_dim(segment_ids, first_row, query_block, 0)
        scores = jnp.einsum('tkgd,skd->kgts', query_tile, key_full, precision=lax.Precision.HIGHEST) * score_scale
        visible = (every_row[None, :] <= query_rows[:, None]) & (segment_ids[None, :] == query_segs[:, None])
        scores = jnp.where(visible[None, None], scores, masked_score)
        row_max = lax.optimization_barrier(jnp.max(scores, axis=-1, keepdims=True))
        weights_full = jnp.where(visible[None, None], jnp.exp(scores - row_max), 0.0)
        normalizer = lax.optimization_barrier(jnp.sum(weights_full, axis=-1))
        weights_low = lax.optimization_barrier(weights_full.astype(jnp.bfloat16)).astype(jnp.float32)
        numerator = jnp.einsum('kgts,skd->kgtd', weights_low, value_full, precision=lax.Precision.HIGHEST)
        output = numerator / normalizer[..., None]
        return jnp.transpose(output, (2, 0, 1, 3)).reshape(query_block, HEADS * HEAD_DIM).astype(jnp.bfloat16)
    attended = lax.map(attend, jnp.arange(TOKENS // query_block, dtype=jnp.int32)).reshape(TOKENS, HEADS * HEAD_DIM)
    head_width = HEADS * HEAD_DIM // N_TP
    summed = jnp.zeros((TOKENS, OUT_WIDTH), jnp.float32)
    for shard in range(N_TP):
        term = jnp.dot(attended[:, shard * head_width:(shard + 1) * head_width], out_weight[shard * head_width:(shard + 1) * head_width], preferred_element_type=jnp.float32).astype(jnp.bfloat16)
        summed = summed + lax.optimization_barrier(term).astype(jnp.float32)
    return summed.astype(jnp.bfloat16)
```

```python
import functools
import math

import jax
import jax.numpy as jnp
import numpy as np
from jax import lax
from jax.experimental import pallas as pl
from jax.experimental.pallas import tpu as pltpu
from jax.sharding import PartitionSpec as P

HEADS = 32
KV_HEADS = 4
HEAD_DIM = 128
SEGMENTS = 16

rope_base = 500000.0
masked_score = -1e30
MESH = pl.DeviceIdType.MESH


def to_column(row_values, count):
    down = lax.broadcasted_iota(jnp.int32, (count, count), 0)
    across = lax.broadcasted_iota(jnp.int32, (count, count), 1)
    return jnp.sum(jnp.where(down == across, row_values, 0.0), axis=1, keepdims=True)


def doc_start_column(seg_all, block, members, rows):
    own = to_column(seg_all[block].astype(jnp.float32), rows)
    earlier = jnp.zeros((rows, rows), jnp.float32)
    for member in range(members):
        earlier = earlier + jnp.where(seg_all[member].astype(jnp.float32) < own, 1.0, 0.0)
    return jnp.sum(earlier, axis=1, keepdims=True)


def layer_kernel(
    members, slots, inverse_ref, q_ref, k_ref, v_ref, seg_ref, w_hbm, out_ref,
    seg_all, k_all, v_all, q_all, w_all, attended, top, total, acc,
    half_send, half_recv, half_own, piece, recv,
    seg_ss, seg_rs, k_ss, k_rs, v_ss, v_rs, q_ss, q_rs, w_ss, w_rs, own_sem,
    d_ss, d_rs, c_ss, c_rs,
):
    rows = q_ref.shape[0]
    heads = q_ref.shape[1] // HEAD_DIM
    width = w_hbm.shape[1]
    half = out_ref.shape[1] // 2
    tp_count = slots
    per = members // slots
    me = lax.axis_index("seq")
    g = lax.axis_index("tp")
    slot = lax.div(me, per)
    place = lax.rem(me, per)
    core = lax.rem(g, 2)
    sibling = g + 1 - 2 * core
    chunk_count = w_ss.shape[0] // max(per - 1, 1)
    chunk_rows = w_hbm.shape[0] // chunk_count

    barrier = pltpu.get_barrier_semaphore()
    for d in range(1, members):
        pl.semaphore_signal(
            barrier, inc=1, device_id={"seq": lax.rem(me + d, members)}, device_id_type=MESH
        )
    for e in range(1, tp_count):
        for d in range(slots):
            pl.semaphore_signal(
                barrier,
                inc=1,
                device_id={
                    "seq": lax.rem(slot + d, slots) * per + place,
                    "tp": lax.rem(g + e, tp_count),
                },
                device_id_type=MESH,
            )

    own_columns = pl.ds(pl.multiple_of(place * width, width), width)
    own_weight = pltpu.make_async_copy(w_hbm, w_all.at[:, own_columns], own_sem)
    own_weight.start()

    pl.semaphore_wait(barrier, members - 1 + (tp_count - 1) * slots)

    def to_member(source, target, send, recv_sem, d):
        return pltpu.make_async_remote_copy(
            src_ref=source,
            dst_ref=target,
            send_sem=send.at[d - 1],
            recv_sem=recv_sem.at[d - 1],
            device_id={"seq": lax.rem(me + d, members)},
            device_id_type=MESH,
        )

    my_tile = lax.div(me, 2)
    my_part = pl.ds(pl.multiple_of(lax.rem(me, 2) * rows, rows), rows)
    pending = []

    seg_copies = [to_member(seg_ref, seg_all.at[me], seg_ss, seg_rs, d) for d in range(1, members)]
    for copy in seg_copies:
        copy.start()
    v_copies = [
        to_member(v_ref, v_all.at[my_tile, my_part], v_ss, v_rs, d) for d in range(1, members)
    ]
    for copy in v_copies:
        copy.start()

    w_copies = []
    for c in range(chunk_count):
        band = pl.ds(c * chunk_rows, chunk_rows)
        for r in range(1, per):
            peer = slot * per + lax.rem(place + r, per)
            w_copies.append(
                pltpu.make_async_remote_copy(
                    src_ref=w_hbm.at[band],
                    dst_ref=w_all.at[band, own_columns],
                    send_sem=w_ss.at[c * (per - 1) + r - 1],
                    recv_sem=w_rs.at[c * (per - 1) + r - 1],
                    device_id={"seq": peer},
                    device_id_type=MESH,
                )
            )
    for copy in w_copies[: per - 1]:
        copy.start()

    seg_all[me] = seg_ref[...]
    v_all[my_tile, my_part] = v_ref[...]
    for copy in seg_copies:
        copy.wait_recv()

    row_index = lax.broadcasted_iota(jnp.int32, (rows, 1), 0)
    position = (me * rows + row_index).astype(jnp.float32) - doc_start_column(
        seg_all, me, members, rows
    )
    angle = position * inverse_ref[...]
    cosine = jnp.cos(angle)
    lane = lax.broadcasted_iota(jnp.int32, (rows, HEAD_DIM), 1)
    sine = jnp.where(lane < HEAD_DIM // 2, -1.0, 1.0) * jnp.sin(angle)

    def rotated(values):
        wide = values.astype(jnp.float32)
        return (wide * cosine + pltpu.roll(wide, HEAD_DIM // 2, 1) * sine).astype(jnp.bfloat16)

    k_all[my_tile, my_part] = rotated(k_ref[...])
    k_own = k_all.at[my_tile, my_part]
    k_copies = [to_member(k_own, k_own, k_ss, k_rs, d) for d in range(1, members)]
    for copy in k_copies:
        copy.start()
    for head in range(heads):
        lanes = slice(head * HEAD_DIM, (head + 1) * HEAD_DIM)
        q_all[slot, :, lanes] = rotated(q_ref[:, lanes])
    q_copies = []
    for d in range(1, slots):
        peer = lax.rem(slot + slots - d, slots) * per + place
        q_copies.append(
            pltpu.make_async_remote_copy(
                src_ref=q_all.at[slot],
                dst_ref=q_all.at[slot],
                send_sem=q_ss.at[d - 1],
                recv_sem=q_rs.at[d - 1],
                device_id={"seq": peer},
                device_id_type=MESH,
            )
        )
    for copy in q_copies:
        copy.start()
    for copy in w_copies[per - 1 :]:
        copy.start()

    for copy in v_copies:
        copy.wait_recv()
    for copy in k_copies:
        copy.wait_recv()

    tile_rows = k_all.shape[1]
    reach = -(-(3 * members * rows // 4 - 1) // rows)
    score_scale = math.log2(math.e) / math.sqrt(HEAD_DIM)

    def attend(block_slot):
        block = block_slot * per + place
        start = doc_start_column(seg_all, block, members, rows).astype(jnp.int32)
        query_index = block * rows + lax.broadcasted_iota(jnp.int32, (rows, tile_rows), 0)
        top[...] = jnp.full(top.shape, 0.5 * masked_score, jnp.float32)
        total[...] = jnp.zeros(total.shape, jnp.float32)
        acc[...] = jnp.zeros(acc.shape, jnp.float32)

        def tile(number, unused):
            key_index = number * tile_rows + lax.broadcasted_iota(
                jnp.int32, (rows, tile_rows), 1
            )
            visible = (key_index <= query_index) & (key_index >= start)
            bias = jnp.where(visible, 0.0, masked_score)
            key_tile = k_all[number]
            value_tile = v_all[number]
            for head in range(heads):
                lanes = slice(head * HEAD_DIM, (head + 1) * HEAD_DIM)
                scores = lax.dot_general(
                    q_all[block_slot, :, lanes],
                    key_tile,
                    (((1,), (1,)), ((), ())),
                    preferred_element_type=jnp.float32,
                )
                scores = scores * score_scale + bias
                old = top[head]
                new = jnp.maximum(old, jnp.max(scores, axis=1, keepdims=True))
                rescale = jnp.exp2(old - new)
                weights = jnp.exp2(
                    scores - jnp.concatenate([new] * (tile_rows // HEAD_DIM), axis=1)
                )
                added = weights[:, :HEAD_DIM]
                for part in range(1, tile_rows // HEAD_DIM):
                    added = added + weights[:, part * HEAD_DIM : (part + 1) * HEAD_DIM]
                top[head] = new
                total[head] = total[head] * rescale + added
                acc[head] = acc[head] * rescale + jnp.dot(
                    weights.astype(jnp.bfloat16), value_tile, preferred_element_type=jnp.float32
                )
            return unused

        first = lax.div(jnp.maximum(block - reach, 0), 2)
        lax.fori_loop(first, lax.div(block, 2) + 1, tile, 0)
        for head in range(heads):
            attended[block_slot, :, head * HEAD_DIM : (head + 1) * HEAD_DIM] = (
                acc[head] / jnp.sum(total[head], axis=1, keepdims=True)
            ).astype(jnp.bfloat16)

    for d in range(slots):
        if d > 0:
            q_copies[d - 1].wait_recv()
        attend(lax.rem(slot + d, slots))

    own_weight.wait()
    for copy in w_copies:
        copy.wait_recv()

    column_step = 256
    y_index = lax.div(g, 2)
    final_columns = pl.ds(pl.multiple_of(core * half, half), half)
    c_copies = []
    for d in list(range(1, slots)) + [0]:
        block_slot = lax.rem(slot + d, slots)
        block = block_slot * per + place
        for c in range(half // column_step):
            local_lanes = slice(c * column_step, (c + 1) * column_step)
            start = pl.multiple_of((1 - core) * half + c * column_step, column_step)
            half_send[d, :, local_lanes] = jnp.dot(
                attended[block_slot],
                w_all[:, pl.ds(start, column_step)],
                preferred_element_type=jnp.float32,
            ).astype(jnp.bfloat16)
        d2d = pltpu.make_async_remote_copy(
            src_ref=half_send.at[d],
            dst_ref=half_recv.at[d],
            send_sem=d_ss.at[d],
            recv_sem=d_rs.at[d],
            device_id={"tp": sibling},
            device_id_type=MESH,
        )
        d2d.start()
        pending.append(d2d)
        for c in range(half // column_step):
            local_lanes = slice(c * column_step, (c + 1) * column_step)
            start = pl.multiple_of(core * half + c * column_step, column_step)
            half_own[:, local_lanes] = jnp.dot(
                attended[block_slot],
                w_all[:, pl.ds(start, column_step)],
                preferred_element_type=jnp.float32,
            )
        d2d.wait_recv()
        piece[d] = (half_own[...] + half_recv[d].astype(jnp.float32)).astype(jnp.bfloat16)
        copy = pltpu.make_async_remote_copy(
            src_ref=piece.at[d],
            dst_ref=recv.at[y_index, :, final_columns],
            send_sem=c_ss.at[d],
            recv_sem=c_rs.at[g],
            device_id={"seq": block, "tp": slot},
            device_id_type=MESH,
        )
        if d > 0:
            copy.start()
        else:
            here = g == slot

            @pl.when(here)
            def _():
                recv[y_index, :, final_columns] = piece[0]

            @pl.when(jnp.logical_not(here))
            def _():
                copy.start()
        c_copies.append(copy)

    for source in range(tp_count):
        arrival = pltpu.make_async_remote_copy(
            src_ref=piece.at[0],
            dst_ref=recv.at[source // 2, :, (source % 2) * half : (source % 2 + 1) * half],
            send_sem=c_ss.at[0],
            recv_sem=c_rs.at[source],
            device_id={"seq": me, "tp": lax.rem(g + 1, tp_count)},
            device_id_type=MESH,
        )

        @pl.when(jnp.logical_or(g != source, g != slot))
        def _():
            arrival.wait_recv()

    result = recv[0].astype(jnp.float32)
    for part in range(1, tp_count // 2):
        result = result + recv[part].astype(jnp.float32)
    out_ref[...] = result.astype(out_ref.dtype)

    for copy in seg_copies + v_copies + k_copies + q_copies + w_copies + pending + c_copies[:-1]:
        copy.wait_send()

    @pl.when(g != slot)
    def _():
        c_copies[-1].wait_send()


def local(queries, keys, values, segment_ids, out_weight):
    rows = queries.shape[0]
    members = lax.axis_size("seq")
    slots = lax.axis_size("tp")
    per = members // slots
    heads = queries.shape[1] // HEAD_DIM
    out_width = out_weight.shape[1] * per
    half = out_width // 2
    chunk_count = 4
    exponent = np.arange(HEAD_DIM // 2, dtype=np.float32) * np.float32(2.0 / HEAD_DIM)
    inverse = np.power(np.float32(rope_base), -exponent).astype(np.float32)
    inverse = jnp.asarray(np.concatenate([inverse, inverse])[None, :])
    vmem = pl.BlockSpec(memory_space=pltpu.VMEM)
    bf16, f32 = jnp.bfloat16, jnp.float32
    dma = pltpu.SemaphoreType.DMA
    return pl.pallas_call(
        functools.partial(layer_kernel, members, slots),
        out_shape=jax.ShapeDtypeStruct((rows, out_width), bf16),
        in_specs=[vmem] * 5 + [pl.BlockSpec(memory_space=pl.ANY)],
        out_specs=vmem,
        scratch_shapes=[
            pltpu.VMEM((members, 1, rows), jnp.int32),
            pltpu.VMEM((members // 2, 2 * rows, HEAD_DIM), bf16),
            pltpu.VMEM((members // 2, 2 * rows, HEAD_DIM), bf16),
            pltpu.VMEM((slots, rows, queries.shape[1]), bf16),
            pltpu.VMEM((out_weight.shape[0], out_width), bf16),
            pltpu.VMEM((slots, rows, queries.shape[1]), bf16),
            pltpu.VMEM((heads, rows, HEAD_DIM), f32),
            pltpu.VMEM((heads, rows, HEAD_DIM), f32),
            pltpu.VMEM((heads, rows, HEAD_DIM), f32),
            pltpu.VMEM((slots, rows, half), bf16),
            pltpu.VMEM((slots, rows, half), bf16),
            pltpu.VMEM((rows, half), f32),
            pltpu.VMEM((slots, rows, half), bf16),
            pltpu.VMEM((slots // 2, rows, out_width), bf16),
        ]
        + [dma((members - 1,))] * 6
        + [dma((slots - 1,))] * 2
        + [dma((chunk_count * (per - 1),))] * 2
        + [dma(())]
        + [dma((slots,))] * 4,
        compiler_params=pltpu.CompilerParams(
            collective_id=0, has_side_effects=True, vmem_limit_bytes=60 * 1024 * 1024
        ),
    )(inverse, queries, keys, values, segment_ids.reshape(1, rows), out_weight)


def solution(mesh):
    return jax.shard_map(
        local,
        mesh=mesh,
        in_specs=(P("seq", "tp"), P("seq", "tp"), P("seq", "tp"), P("seq"), P("tp", "seq")),
        out_specs=P("seq", "tp"),
        check_vma=False,
    )
```

```python
import functools
import math

import jax
import jax.numpy as jnp
import numpy as np
from jax import lax
from jax.experimental import pallas as pl
from jax.experimental.pallas import tpu as pltpu
from jax.sharding import PartitionSpec as P

HEADS = 32
KV_HEADS = 4
HEAD_DIM = 128
SEGMENTS = 16

rope_base = 500000.0
masked_score = -1e30
MESH = pl.DeviceIdType.MESH


def to_column(row_values, count):
    down = lax.broadcasted_iota(jnp.int32, (count, count), 0)
    across = lax.broadcasted_iota(jnp.int32, (count, count), 1)
    return jnp.sum(jnp.where(down == across, row_values, 0.0), axis=1, keepdims=True)


def doc_start_column(seg_all, block, members, rows):
    own = to_column(seg_all[block].astype(jnp.float32), rows)
    earlier = jnp.zeros((rows, rows), jnp.float32)
    for member in range(members):
        earlier = earlier + jnp.where(seg_all[member].astype(jnp.float32) < own, 1.0, 0.0)
    return jnp.sum(earlier, axis=1, keepdims=True)


def layer_kernel(
    members, slots, inverse_hbm, q_hbm, k_hbm, v_hbm, seg_hbm, w_hbm, recv,
    inverse_ref, q_ref, k_ref, seg_all, k_all, v_all, q_all, w_all, attended,
    top, total, acc, scores_ref, half_send, half_recv, half_own, piece, in_sems,
    seg_ss, seg_rs, k_ss, k_rs, v_ss, v_rs, k2_ss, k2_rs, v2_ss, v2_rs, q_ss, q_rs,
    w_ss, w_rs, own_sem, d_ss, d_rs, c_ss, c_rs,
):
    rows = q_ref.shape[0]
    heads = q_ref.shape[1] // HEAD_DIM
    width = w_hbm.shape[1]
    out_width = recv.shape[2]
    tp_count = slots
    per = members // slots
    me = lax.axis_index("seq")
    g = lax.axis_index("tp")
    slot = lax.div(me, per)
    place = lax.rem(me, per)
    core = lax.rem(g, 2)
    sibling = g + 1 - 2 * core
    chunk_count = w_ss.shape[0] // (per - 1)

    def part_of(ref, block):
        return ref.at[
            lax.div(block, 2), pl.ds(pl.multiple_of(lax.rem(block, 2) * rows, rows), rows)
        ]

    inputs = [
        (seg_hbm, seg_all.at[me]),
        (v_hbm, part_of(v_all, me)),
        (k_hbm, k_ref),
        (inverse_hbm, inverse_ref),
        (q_hbm, q_ref),
    ]
    inputs = [
        pltpu.make_async_copy(source, target, in_sems.at[i])
        for i, (source, target) in enumerate(inputs)
    ]
    for copy in inputs:
        copy.start()

    barrier = pltpu.get_barrier_semaphore()
    for d in range(1, members):
        pl.semaphore_signal(
            barrier, inc=1, device_id={"seq": lax.rem(me + d, members)}, device_id_type=MESH
        )
    for e in range(1, tp_count):
        for d in range(slots):
            pl.semaphore_signal(
                barrier,
                inc=1,
                device_id={
                    "seq": lax.rem(slot + d, slots) * per + place,
                    "tp": lax.rem(g + e, tp_count),
                },
                device_id_type=MESH,
            )

    own_columns = pl.ds(pl.multiple_of(place * width, width), width)
    own_weight = pltpu.make_async_copy(w_hbm, w_all.at[:, own_columns], own_sem)
    own_weight.start()
    for copy in inputs:
        copy.wait()

    with jax.named_scope("barrier_wait"):
        pl.semaphore_wait(barrier, members - 1 + (tp_count - 1) * slots)

    def send(source, target, send_sem, recv_sem, peer):
        return pltpu.make_async_remote_copy(
            src_ref=source,
            dst_ref=target,
            send_sem=send_sem,
            recv_sem=recv_sem,
            device_id={"seq": peer},
            device_id_type=MESH,
        )

    def from_slot(d):
        return lax.rem(slot + slots - d, slots) * per + place

    def to_slots(source, target, ss, rs):
        return [
            send(source, target, ss.at[d - 1], rs.at[d - 1], lax.rem(slot + d, slots) * per + place)
            for d in range(1, slots)
        ]

    def relay(ref, d, ss, rs):
        block = from_slot(d)
        return [
            send(
                part_of(ref, block),
                part_of(ref, block),
                ss.at[d * (per - 1) + r - 1],
                rs.at[d * (per - 1) + r - 1],
                slot * per + lax.rem(place + r, per),
            )
            for r in range(1, per)
        ]

    def start_all(copies):
        for copy in copies:
            copy.start()
        return copies

    started = []
    seg_copies = start_all(
        [
            send(seg_all.at[me], seg_all.at[me], seg_ss.at[d - 1], seg_rs.at[d - 1], lax.rem(me + d, members))
            for d in range(1, members)
        ]
    )
    started += seg_copies
    v_own = part_of(v_all, me)
    v_copies = start_all(to_slots(v_own, v_own, v_ss, v_rs))
    started += v_copies
    v_relays = start_all(relay(v_all, 0, v2_ss, v2_rs))

    units = c_rs.shape[1]
    if units > 1:
        unit_width = out_width // units
        own_units = units // per
        unit_starts = [
            lax.rem(place + u // own_units, per) * width + (u % own_units) * unit_width
            for u in range(units)
        ]
    else:
        unit_width, own_units, unit_starts = width, 1, [0]
    half = piece.shape[2]
    column_chunks = width // unit_width
    bands = chunk_count // column_chunks
    band_rows = w_hbm.shape[0] // bands
    w_copies = []
    for c in range(chunk_count):
        band = pl.ds((c % bands) * band_rows, band_rows)
        first = (c // bands) * unit_width
        target_columns = pl.ds(pl.multiple_of(place * width + first, unit_width), unit_width)
        for r in range(1, per):
            w_copies.append(
                send(
                    w_hbm.at[band, first : first + unit_width],
                    w_all.at[band, target_columns],
                    w_ss.at[c * (per - 1) + r - 1],
                    w_rs.at[c * (per - 1) + r - 1],
                    slot * per + lax.rem(place + r, per),
                )
            )
    early = 2 * (per - 1)
    start_all(w_copies[:early])

    with jax.named_scope("seg_wait"):
        for copy in seg_copies:
            copy.wait_recv()

    row_index = lax.broadcasted_iota(jnp.int32, (rows, 1), 0)
    position = (me * rows + row_index).astype(jnp.float32) - doc_start_column(
        seg_all, me, members, rows
    )
    angle = position * inverse_ref[...]
    cosine = jnp.cos(angle)
    lane = lax.broadcasted_iota(jnp.int32, (rows, HEAD_DIM), 1)
    sine = jnp.where(lane < HEAD_DIM // 2, -1.0, 1.0) * jnp.sin(angle)

    def rotated(values):
        wide = values.astype(jnp.float32)
        return (wide * cosine + pltpu.roll(wide, HEAD_DIM // 2, 1) * sine).astype(jnp.bfloat16)

    k_own = part_of(k_all, me)
    k_own[...] = rotated(k_ref[...])
    k_copies = start_all(to_slots(k_own, k_own, k_ss, k_rs))
    started += k_copies
    k_relays = start_all(relay(k_all, 0, k2_ss, k2_rs))

    for head in range(heads):
        lanes = slice(head * HEAD_DIM, (head + 1) * HEAD_DIM)
        q_all[slot, :, lanes] = rotated(q_ref[:, lanes])
    pair = slot + 1 - 2 * lax.rem(slot, 2)
    inner = lax.rem(lax.div(slot + 1, 2), 2)
    third = 2 - lax.div(slot, 2)
    fourth = (slots - 1) * (1 - lax.div(slot, 2))

    def send_queries(block_slot, target_slot, index):
        return send(
            q_all.at[block_slot],
            q_all.at[block_slot],
            q_ss.at[index],
            q_rs.at[block_slot],
            target_slot * per + place,
        )

    first_queries, second_queries = send_queries(slot, pair, 0), send_queries(slot, third, 1)
    first_queries.start()
    started.append(second_queries)

    @pl.when(inner == 1)
    def _():
        second_queries.start()


    for d in range(1, slots):
        with jax.named_scope(f"v_wait{d}"):
            v_copies[d - 1].wait_recv()
        v_relays += start_all(relay(v_all, d, v2_ss, v2_rs))
    for d in range(1, slots):
        with jax.named_scope(f"k_wait{d}"):
            k_copies[d - 1].wait_recv()
        k_relays += start_all(relay(k_all, d, k2_ss, k2_rs))
    started += v_relays + k_relays
    start_all(w_copies[early:])
    with jax.named_scope("kv_relay_wait"):
        for copy in v_relays + k_relays:
            copy.wait_recv()

    tile_rows = k_all.shape[1]
    reach = -(-(3 * members * rows // 4 - 1) // rows)
    score_scale = math.log2(math.e) / math.sqrt(HEAD_DIM)

    group = scores_ref.shape[1]

    def attend(block_slot):
        block = block_slot * per + place
        start = doc_start_column(seg_all, block, members, rows).astype(jnp.int32)
        query_index = block * rows + lax.broadcasted_iota(jnp.int32, (rows, tile_rows), 0)
        first = lax.div(jnp.maximum(block - reach, 0), 2)
        last = lax.div(block, 2) + 1
        parts = [slice(p * HEAD_DIM, (p + 1) * HEAD_DIM) for p in range(tile_rows // HEAD_DIM)]
        for base in range(0, heads, group):
            top[...] = jnp.full(top.shape, masked_score, jnp.float32)
            total[...] = jnp.zeros(total.shape, jnp.float32)
            acc[...] = jnp.zeros(acc.shape, jnp.float32)

            def score_tile(number, unused):
                key_index = number * tile_rows + lax.broadcasted_iota(
                    jnp.int32, (rows, tile_rows), 1
                )
                visible = (key_index <= query_index) & (key_index >= start)
                bias = jnp.where(visible, 0.0, masked_score)
                key_tile = k_all[number]
                for head in range(group):
                    lanes = slice((base + head) * HEAD_DIM, (base + head + 1) * HEAD_DIM)
                    scores = lax.dot_general(
                        q_all[block_slot, :, lanes],
                        key_tile,
                        (((1,), (1,)), ((), ())),
                        preferred_element_type=jnp.float32,
                    )
                    scores = scores * score_scale + bias
                    scores_ref[number, head] = scores
                    best = top[head]
                    for part in parts:
                        best = jnp.maximum(best, scores[:, part])
                    top[head] = best
                return unused

            lax.fori_loop(first, last, score_tile, 0)
            for head in range(group):
                top[head] = jnp.broadcast_to(
                    jnp.max(top[head], axis=1, keepdims=True), (rows, HEAD_DIM)
                )

            def value_tile(number, unused):
                values = v_all[number]
                for head in range(group):
                    weights = jnp.exp2(
                        scores_ref[number, head] - jnp.concatenate([top[head]] * len(parts), axis=1)
                    )
                    added = total[head]
                    for part in parts:
                        added = added + weights[:, part]
                    total[head] = added
                    acc[head] = acc[head] + jnp.dot(
                        weights.astype(jnp.bfloat16), values, preferred_element_type=jnp.float32
                    )
                return unused

            lax.fori_loop(first, last, value_tile, 0)
            for head in range(group):
                lanes = slice((base + head) * HEAD_DIM, (base + head + 1) * HEAD_DIM)
                attended[block_slot, :, lanes] = (
                    acc[head] / jnp.sum(total[head], axis=1, keepdims=True)
                ).astype(jnp.bfloat16)

    y_index = lax.div(g, 2)
    step = min(256, half)
    pair_copies, c_copies = [], []
    held = []

    def multiply(block_slot, unit, order):
        index = order * units + unit
        buffer = len(pair_copies) % half_own.shape[0]
        kept = unit_starts[unit] + core * half
        given = unit_starts[unit] + (1 - core) * half
        for c in range(half // step):
            half_send[index, :, c * step : (c + 1) * step] = jnp.dot(
                attended[block_slot],
                w_all[:, pl.ds(pl.multiple_of(given + c * step, step), step)],
                preferred_element_type=jnp.float32,
            ).astype(jnp.bfloat16)
        across = pltpu.make_async_remote_copy(
            src_ref=half_send.at[index],
            dst_ref=half_recv.at[index],
            send_sem=d_ss.at[index],
            recv_sem=d_rs.at[index],
            device_id={"tp": sibling},
            device_id_type=MESH,
        )
        across.start()
        pair_copies.append(across)
        for c in range(half // step):
            half_own[buffer, :, c * step : (c + 1) * step] = jnp.dot(
                attended[block_slot],
                w_all[:, pl.ds(pl.multiple_of(kept + c * step, step), step)],
                preferred_element_type=jnp.float32,
            )
        held.append((block_slot, unit, order, index, buffer, kept, across))

    def finish():
        block_slot, unit, order, index, buffer, kept, across = held.pop(0)
        with jax.named_scope(f"across_wait{index}"):
            across.wait_recv()
        piece[index] = (half_own[buffer] + half_recv[index].astype(jnp.float32)).astype(
            jnp.bfloat16
        )
        target = recv.at[y_index, :, pl.ds(pl.multiple_of(kept, half), half)]
        copy = pltpu.make_async_remote_copy(
            src_ref=piece.at[index],
            dst_ref=target,
            send_sem=c_ss.at[index],
            recv_sem=c_rs.at[g, unit],
            device_id={"seq": block_slot * per + place, "tp": slot},
            device_id_type=MESH,
        )
        if order == 0:

            @pl.when(g == slot)
            def _():
                target[...] = piece[index]

            @pl.when(g != slot)
            def _():
                copy.start()
        else:
            copy.start()
        c_copies.append((order, copy))

    def pass_on(block_slot, index):
        copy = send_queries(block_slot, pair, index)

        @pl.when(inner == 1)
        def _():
            with jax.named_scope(f"forward_wait{index}"):
                copy.wait_recv()
            copy.start()

        return copy

    slot_order = [slot, pair, third, fourth]
    query_forwards = []
    for order, block_slot in enumerate(slot_order):
        if order > 0:
            arrived = send_queries(block_slot, pair, 0)
            if order == 1:
                with jax.named_scope(f"q_wait{order}"):
                    arrived.wait_recv()
            else:

                @pl.when(inner == 0)
                def _():
                    with jax.named_scope(f"q_wait{order}"):
                        arrived.wait_recv()
        with jax.named_scope(f"attend{order}"):
            attend(block_slot)
        if order == 0:
            own_weight.wait()
        if units > 1:
            with jax.named_scope(f"product{order}"):
                for unit in range(own_units):
                    multiply(block_slot, unit, order)
                    if len(held) > 1:
                        finish()
                while held:
                    finish()
        if order == 0:
            first_queries.wait_send()

            @pl.when(inner == 0)
            def _():
                second_queries.start()

            query_forwards.append(pass_on(third, 2))
        if order == 1:
            query_forwards.append(pass_on(fourth, 3))

    late = own_units if units > 1 else 0
    for unit in range(late, units):
        chunk = (unit % own_units) * bands
        sender = unit // own_units - 1
        with jax.named_scope(f"w_wait{unit}"):
            for c in range(chunk_count):
                for r in range(per - 1):
                    if units == 1 or (chunk <= c < chunk + bands and r == per - 2 - sender):
                        w_copies[c * (per - 1) + r].wait_recv()
        for order in list(range(1, slots)) + [0]:
            multiply(slot_order[order], unit, order)
            if len(held) > 1:
                finish()
    while held:
        finish()

    for source in range(tp_count):
        for unit in range(units):
            arrival = pltpu.make_async_remote_copy(
                src_ref=piece.at[0],
                dst_ref=recv.at[source // 2, :, :half],
                send_sem=c_ss.at[0],
                recv_sem=c_rs.at[source, unit],
                device_id={"seq": me, "tp": sibling},
                device_id_type=MESH,
            )

            @pl.when(jnp.logical_or(g != source, g != slot))
            def _():
                with jax.named_scope(f"arrive{source}_{unit}"):
                    arrival.wait_recv()

    with jax.named_scope("send_waits"):
        for copy in started + w_copies + pair_copies:
            copy.wait_send()
        for order, copy in c_copies:
            if order > 0:
                copy.wait_send()

        @pl.when(g != slot)
        def _():
            for order, copy in c_copies:
                if order == 0:
                    copy.wait_send()

        @pl.when(inner == 1)
        def _():
            for copy in query_forwards:
                copy.wait_send()


def add_kernel(pieces, out_ref):
    result = pieces[0].astype(jnp.float32)
    for part in range(1, pieces.shape[0]):
        result = result + pieces[part].astype(jnp.float32)
    out_ref[...] = result.astype(out_ref.dtype)


def local(queries, keys, values, segment_ids, out_weight):
    rows = queries.shape[0]
    members = lax.axis_size("seq")
    slots = lax.axis_size("tp")
    per = members // slots
    heads = queries.shape[1] // HEAD_DIM
    out_width = out_weight.shape[1] * per
    units = out_width // 512 if out_weight.shape[1] % 512 == 0 else 1
    half = out_width // units // 2
    chunk_count = 16
    tiles = members // 2
    group = heads
    while group > 1 and tiles * group * rows * 2 * rows * 4 > 20 * 1024 * 1024:
        group //= 2
    exponent = np.arange(HEAD_DIM // 2, dtype=np.float32) * np.float32(2.0 / HEAD_DIM)
    inverse = np.power(np.float32(rope_base), -exponent).astype(np.float32)
    inverse = jnp.asarray(np.concatenate([inverse, inverse])[None, :])
    vmem = pl.BlockSpec(memory_space=pltpu.VMEM)
    bf16, f32 = jnp.bfloat16, jnp.float32
    dma = pltpu.SemaphoreType.DMA
    pieces = pl.pallas_call(
        functools.partial(layer_kernel, members, slots),
        out_shape=jax.ShapeDtypeStruct((slots // 2, rows, out_width), bf16),
        in_specs=[pl.BlockSpec(memory_space=pl.ANY)] * 6,
        out_specs=vmem,
        scratch_shapes=[
            pltpu.VMEM((1, HEAD_DIM), f32),
            pltpu.VMEM(queries.shape, bf16),
            pltpu.VMEM(keys.shape, bf16),
            pltpu.VMEM((members, 1, rows), jnp.int32),
            pltpu.VMEM((tiles, 2 * rows, HEAD_DIM), bf16),
            pltpu.VMEM((tiles, 2 * rows, HEAD_DIM), bf16),
            pltpu.VMEM((slots, rows, queries.shape[1]), bf16),
            pltpu.VMEM((out_weight.shape[0], out_width), bf16),
            pltpu.VMEM((slots, rows, queries.shape[1]), bf16),
            pltpu.VMEM((group, rows, HEAD_DIM), f32),
            pltpu.VMEM((group, rows, HEAD_DIM), f32),
            pltpu.VMEM((group, rows, HEAD_DIM), f32),
            pltpu.VMEM((tiles, group, rows, 2 * rows), f32),
            pltpu.VMEM((slots * units, rows, half), bf16),
            pltpu.VMEM((slots * units, rows, half), bf16),
            pltpu.VMEM((2, rows, half), f32),
            pltpu.VMEM((slots * units, rows, half), bf16),
            dma((5,)),
        ]
        + [dma((members - 1,))] * 2
        + [dma((slots - 1,))] * 4
        + [dma((slots * (per - 1),))] * 4
        + [dma((slots,))] * 2
        + [dma((chunk_count * (per - 1),))] * 2
        + [dma(())]
        + [dma((slots * units,))] * 3
        + [dma((slots, units))],
        compiler_params=pltpu.CompilerParams(
            collective_id=0, has_side_effects=True, vmem_limit_bytes=60 * 1024 * 1024
        ),
    )(inverse, queries, keys, values, segment_ids.reshape(1, rows), out_weight)
    band = rows // 4
    return pl.pallas_call(
        add_kernel,
        grid=(rows // band,),
        out_shape=jax.ShapeDtypeStruct((rows, out_width), bf16),
        in_specs=[pl.BlockSpec((slots // 2, band, out_width), lambda i: (0, i, 0))],
        out_specs=pl.BlockSpec((band, out_width), lambda i: (i, 0)),
    )(pieces)


def solution(mesh):
    return jax.shard_map(
        local,
        mesh=mesh,
        in_specs=(P("seq", "tp"), P("seq", "tp"), P("seq", "tp"), P("seq"), P("tp", "seq")),
        out_specs=P("seq", "tp"),
        check_vma=False,
    )
```

```python
import functools
import math

import jax
import jax.numpy as jnp
import numpy as np
from jax import lax
from jax.experimental import pallas as pl
from jax.experimental.pallas import tpu as pltpu
from jax.sharding import PartitionSpec as P

HEADS = 32
KV_HEADS = 4
HEAD_DIM = 128
SEGMENTS = 16

rope_base = 500000.0
masked_score = -1e30
MESH = pl.DeviceIdType.MESH


def to_column(row_values, count):
    down = lax.broadcasted_iota(jnp.int32, (count, count), 0)
    across = lax.broadcasted_iota(jnp.int32, (count, count), 1)
    return jnp.sum(jnp.where(down == across, row_values, 0.0), axis=1, keepdims=True)


def doc_start_column(seg_all, block, members, rows):
    own = to_column(seg_all[block].astype(jnp.float32), rows)
    earlier = jnp.zeros((rows, rows), jnp.float32)
    for member in range(members):
        earlier = earlier + jnp.where(seg_all[member].astype(jnp.float32) < own, 1.0, 0.0)
    return jnp.sum(earlier, axis=1, keepdims=True)


def layer_kernel(
    members, slots, inverse_hbm, q_hbm, k_hbm, v_hbm, seg_hbm, w_hbm, recv,
    inverse_ref, q_ref, k_ref, seg_all, k_all, v_all, q_all, w_all, attended,
    top, total, acc, scores_ref, half_send, half_recv, half_own, piece, in_sems,
    seg_ss, seg_rs, k_ss, k_rs, v_ss, v_rs, k2_ss, k2_rs, v2_ss, v2_rs, q_ss, q_rs,
    w_ss, w_rs, own_sem, clear, d_ss, d_rs, c_ss, c_rs,
):
    rows = q_ref.shape[0]
    heads = q_ref.shape[1] // HEAD_DIM
    width = w_hbm.shape[1]
    out_width = recv.shape[2]
    tp_count = slots
    per = members // slots
    me = lax.axis_index("seq")
    g = lax.axis_index("tp")
    slot = lax.div(me, per)
    place = lax.rem(me, per)
    core = lax.rem(g, 2)
    sibling = g + 1 - 2 * core
    chunk_count = w_ss.shape[0] // (per - 1)

    def part_of(ref, block):
        return ref.at[
            lax.div(block, 2), pl.ds(pl.multiple_of(lax.rem(block, 2) * rows, rows), rows)
        ]

    inputs = [
        (seg_hbm, seg_all.at[me]),
        (v_hbm, part_of(v_all, me)),
        (k_hbm, k_ref),
        (inverse_hbm, inverse_ref),
        (q_hbm, q_ref),
    ]
    inputs = [
        pltpu.make_async_copy(source, target, in_sems.at[i])
        for i, (source, target) in enumerate(inputs)
    ]
    for copy in inputs:
        copy.start()

    barrier = pltpu.get_barrier_semaphore()
    for d in range(1, members):
        pl.semaphore_signal(
            barrier, inc=1, device_id={"seq": lax.rem(me + d, members)}, device_id_type=MESH
        )
    for e in range(1, tp_count):
        for d in range(slots):
            pl.semaphore_signal(
                barrier,
                inc=1,
                device_id={
                    "seq": lax.rem(slot + d, slots) * per + place,
                    "tp": lax.rem(g + e, tp_count),
                },
                device_id_type=MESH,
            )

    own_columns = pl.ds(pl.multiple_of(place * width, width), width)
    own_weight = pltpu.make_async_copy(w_hbm, w_all.at[:, own_columns], own_sem)
    own_weight.start()
    for copy in inputs:
        copy.wait()

    with jax.named_scope("barrier_wait"):
        pl.semaphore_wait(barrier, members - 1 + (tp_count - 1) * slots)

    def send(source, target, send_sem, recv_sem, peer):
        return pltpu.make_async_remote_copy(
            src_ref=source,
            dst_ref=target,
            send_sem=send_sem,
            recv_sem=recv_sem,
            device_id={"seq": peer},
            device_id_type=MESH,
        )

    def from_slot(d):
        return lax.rem(slot + slots - d, slots) * per + place

    def to_slots(source, target, ss, rs):
        return [
            send(source, target, ss.at[d - 1], rs.at[d - 1], lax.rem(slot + d, slots) * per + place)
            for d in range(1, slots)
        ]

    def relay(ref, d, ss, rs):
        block = from_slot(d)
        return [
            send(
                part_of(ref, block),
                part_of(ref, block),
                ss.at[d * (per - 1) + r - 1],
                rs.at[d * (per - 1) + r - 1],
                slot * per + lax.rem(place + r, per),
            )
            for r in range(1, per)
        ]

    def start_all(copies):
        for copy in copies:
            copy.start()
        return copies

    started = []
    seg_copies = start_all(
        [
            send(seg_all.at[me], seg_all.at[me], seg_ss.at[d - 1], seg_rs.at[d - 1], lax.rem(me + d, members))
            for d in range(1, members)
        ]
    )
    started += seg_copies
    v_own = part_of(v_all, me)
    v_copies = start_all(to_slots(v_own, v_own, v_ss, v_rs))
    started += v_copies
    v_relays = start_all(relay(v_all, 0, v2_ss, v2_rs))

    units = c_rs.shape[1]
    if units > 1:
        unit_width = out_width // units
        own_units = units // per
        unit_starts = [
            lax.rem(place + u // own_units, per) * width + (u % own_units) * unit_width
            for u in range(units)
        ]
    else:
        unit_width, own_units, unit_starts = width, 1, [0]
    half = piece.shape[2]
    column_chunks = width // unit_width
    bands = chunk_count // column_chunks
    band_rows = w_hbm.shape[0] // bands
    w_copies = []
    for c in range(chunk_count):
        band = pl.ds((c % bands) * band_rows, band_rows)
        first = (c // bands) * unit_width
        target_columns = pl.ds(pl.multiple_of(place * width + first, unit_width), unit_width)
        for r in range(1, per):
            w_copies.append(
                send(
                    w_hbm.at[band, first : first + unit_width],
                    w_all.at[band, target_columns],
                    w_ss.at[c * (per - 1) + r - 1],
                    w_rs.at[c * (per - 1) + r - 1],
                    slot * per + lax.rem(place + r, per),
                )
            )
    early = per - 1
    start_all(w_copies[:early])

    with jax.named_scope("seg_wait"):
        for copy in seg_copies:
            copy.wait_recv()

    row_index = lax.broadcasted_iota(jnp.int32, (rows, 1), 0)
    position = (me * rows + row_index).astype(jnp.float32) - doc_start_column(
        seg_all, me, members, rows
    )
    angle = position * inverse_ref[...]
    cosine = jnp.cos(angle)
    lane = lax.broadcasted_iota(jnp.int32, (rows, HEAD_DIM), 1)
    sine = jnp.where(lane < HEAD_DIM // 2, -1.0, 1.0) * jnp.sin(angle)

    def rotated(values):
        wide = values.astype(jnp.float32)
        return (wide * cosine + pltpu.roll(wide, HEAD_DIM // 2, 1) * sine).astype(jnp.bfloat16)

    k_own = part_of(k_all, me)
    k_own[...] = rotated(k_ref[...])
    k_copies = start_all(to_slots(k_own, k_own, k_ss, k_rs))
    started += k_copies
    k_relays = start_all(relay(k_all, 0, k2_ss, k2_rs))

    for head in range(heads):
        lanes = slice(head * HEAD_DIM, (head + 1) * HEAD_DIM)
        q_all[slot, :, lanes] = rotated(q_ref[:, lanes])
    pair = slot + 1 - 2 * lax.rem(slot, 2)
    inner = lax.rem(lax.div(slot + 1, 2), 2)
    third = 2 - lax.div(slot, 2)
    fourth = (slots - 1) * (1 - lax.div(slot, 2))

    def send_queries(block_slot, target_slot, index):
        return send(
            q_all.at[block_slot],
            q_all.at[block_slot],
            q_ss.at[index],
            q_rs.at[block_slot],
            target_slot * per + place,
        )

    first_queries, second_queries = send_queries(slot, pair, 0), send_queries(slot, third, 1)
    first_queries.start()
    started.append(first_queries)

    @pl.when(inner == 1)
    def _():
        second_queries.start()


    for d in range(1, slots):
        with jax.named_scope(f"v_wait{d}"):
            v_copies[d - 1].wait_recv()
        v_relays += start_all(relay(v_all, d, v2_ss, v2_rs))
    for d in range(1, slots):
        with jax.named_scope(f"k_wait{d}"):
            k_copies[d - 1].wait_recv()
        k_relays += start_all(relay(k_all, d, k2_ss, k2_rs))
    started += v_relays + k_relays
    start_all(w_copies[early:])
    with jax.named_scope("kv_relay_wait"):
        for copy in v_relays + k_relays:
            copy.wait_recv()

    tile_rows = k_all.shape[1]
    reach = -(-(3 * members * rows // 4 - 1) // rows)
    score_scale = math.log2(math.e) / math.sqrt(HEAD_DIM)

    group = scores_ref.shape[1]

    def attend(block_slot):
        block = block_slot * per + place
        start = doc_start_column(seg_all, block, members, rows).astype(jnp.int32)
        query_index = block * rows + lax.broadcasted_iota(jnp.int32, (rows, tile_rows), 0)
        first = lax.div(jnp.maximum(block - reach, 0), 2)
        last = lax.div(block, 2) + 1
        parts = [slice(p * HEAD_DIM, (p + 1) * HEAD_DIM) for p in range(tile_rows // HEAD_DIM)]
        for base in range(0, heads, group):
            top[...] = jnp.full(top.shape, masked_score, jnp.float32)
            total[...] = jnp.zeros(total.shape, jnp.float32)
            acc[...] = jnp.zeros(acc.shape, jnp.float32)

            def score_tile(number, unused):
                key_index = number * tile_rows + lax.broadcasted_iota(
                    jnp.int32, (rows, tile_rows), 1
                )
                visible = (key_index <= query_index) & (key_index >= start)
                bias = jnp.where(visible, 0.0, masked_score)
                key_tile = k_all[number]
                for head in range(group):
                    lanes = slice((base + head) * HEAD_DIM, (base + head + 1) * HEAD_DIM)
                    scores = lax.dot_general(
                        q_all[block_slot, :, lanes],
                        key_tile,
                        (((1,), (1,)), ((), ())),
                        preferred_element_type=jnp.float32,
                    )
                    scores = scores * score_scale + bias
                    scores_ref[number, head] = scores
                    best = top[head]
                    for part in parts:
                        best = jnp.maximum(best, scores[:, part])
                    top[head] = best
                return unused

            lax.fori_loop(first, last, score_tile, 0)
            for head in range(group):
                top[head] = jnp.broadcast_to(
                    jnp.max(top[head], axis=1, keepdims=True), (rows, HEAD_DIM)
                )

            def value_tile(number, unused):
                values = v_all[number]
                for head in range(group):
                    weights = jnp.exp2(
                        scores_ref[number, head] - jnp.concatenate([top[head]] * len(parts), axis=1)
                    )
                    added = total[head]
                    for part in parts:
                        added = added + weights[:, part]
                    total[head] = added
                    acc[head] = acc[head] + jnp.dot(
                        weights.astype(jnp.bfloat16), values, preferred_element_type=jnp.float32
                    )
                return unused

            lax.fori_loop(first, last, value_tile, 0)
            for head in range(group):
                lanes = slice((base + head) * HEAD_DIM, (base + head + 1) * HEAD_DIM)
                attended[block_slot, :, lanes] = (
                    acc[head] / jnp.sum(total[head], axis=1, keepdims=True)
                ).astype(jnp.bfloat16)

    y_index = lax.div(g, 2)
    step = min(256, half)
    pair_copies, c_copies = [], []
    held = []

    def multiply(block_slot, unit, order):
        index = order * units + unit
        buffer = len(pair_copies) % half_own.shape[0]
        kept = unit_starts[unit] + core * half
        given = unit_starts[unit] + (1 - core) * half
        for c in range(half // step):
            half_send[index, :, c * step : (c + 1) * step] = jnp.dot(
                attended[block_slot],
                w_all[:, pl.ds(pl.multiple_of(given + c * step, step), step)],
                preferred_element_type=jnp.float32,
            ).astype(jnp.bfloat16)
        across = pltpu.make_async_remote_copy(
            src_ref=half_send.at[index],
            dst_ref=half_recv.at[index],
            send_sem=d_ss.at[index],
            recv_sem=d_rs.at[index],
            device_id={"tp": sibling},
            device_id_type=MESH,
        )
        across.start()
        pair_copies.append(across)
        for c in range(half // step):
            half_own[buffer, :, c * step : (c + 1) * step] = jnp.dot(
                attended[block_slot],
                w_all[:, pl.ds(pl.multiple_of(kept + c * step, step), step)],
                preferred_element_type=jnp.float32,
            )
        held.append((block_slot, unit, order, index, buffer, kept, across))

    def finish():
        block_slot, unit, order, index, buffer, kept, across = held.pop(0)
        with jax.named_scope(f"across_wait{index}"):
            across.wait_recv()
        piece[index] = (half_own[buffer] + half_recv[index].astype(jnp.float32)).astype(
            jnp.bfloat16
        )
        target = recv.at[y_index, :, pl.ds(pl.multiple_of(kept, half), half)]
        copy = pltpu.make_async_remote_copy(
            src_ref=piece.at[index],
            dst_ref=target,
            send_sem=c_ss.at[index],
            recv_sem=c_rs.at[g, unit],
            device_id={"seq": block_slot * per + place, "tp": slot},
            device_id_type=MESH,
        )
        if order == 0:

            @pl.when(g == slot)
            def _():
                target[...] = piece[index]

            @pl.when(g != slot)
            def _():
                copy.start()
        else:
            copy.start()
        c_copies.append((order, copy))

    def pass_on(block_slot, index):
        copy = send_queries(block_slot, pair, index)

        @pl.when(inner == 1)
        def _():
            with jax.named_scope(f"forward_wait{index}"):
                copy.wait_recv()
            copy.start()

        return copy

    def own_products(block_slot, order):
        if units > 1:
            with jax.named_scope(f"product{order}"):
                for unit in range(own_units):
                    multiply(block_slot, unit, order)
                    if len(held) > 1:
                        finish()
                while held:
                    finish()

    second_block = pair + inner * (third - pair)
    third_block = third + inner * (fourth - third)
    fourth_block = fourth + inner * (pair - fourth)
    query_forwards = []

    def wait_queries(block_slot, only_outer=False):
        arrived = send_queries(block_slot, pair, 0)
        if only_outer:

            @pl.when(inner == 0)
            def _():
                with jax.named_scope("q_wait_outer"):
                    arrived.wait_recv()
        else:
            with jax.named_scope("q_wait_last"):
                arrived.wait_recv()

    with jax.named_scope("attend0"):
        attend(slot)

    @pl.when(inner == 1)
    def _():
        with jax.named_scope("second_q_sent"):
            second_queries.wait_send()
        pl.semaphore_signal(
            clear, inc=1, device_id={"seq": pair * per + place}, device_id_type=MESH
        )

    @pl.when(inner == 0)
    def _():
        with jax.named_scope("clear_wait"):
            pl.semaphore_wait(clear, 1)
        second_queries.start()

    query_forwards.append(pass_on(third, 2))
    wait_queries(pair, only_outer=True)
    with jax.named_scope("attend1"):
        attend(second_block)
    own_weight.wait()
    own_products(second_block, 1)
    own_products(slot, 0)
    query_forwards.append(pass_on(fourth, 3))
    wait_queries(third, only_outer=True)
    with jax.named_scope("attend2"):
        attend(third_block)
    own_products(third_block, 2)
    wait_queries(fourth_block)
    with jax.named_scope("attend3"):
        attend(fourth_block)
    own_products(fourth_block, 3)

    late = own_units if units > 1 else 0
    for unit in range(late, units):
        chunk = (unit % own_units) * bands
        sender = unit // own_units - 1
        with jax.named_scope(f"w_wait{unit}"):
            for c in range(chunk_count):
                for r in range(per - 1):
                    if units == 1 or (chunk <= c < chunk + bands and r == per - 2 - sender):
                        w_copies[c * (per - 1) + r].wait_recv()
        for order, block_slot in ((2, third), (3, fourth), (1, pair), (0, slot)):
            multiply(block_slot, unit, order)
            if len(held) > 1:
                finish()
    while held:
        finish()

    for source in range(tp_count):
        for unit in range(units):
            arrival = pltpu.make_async_remote_copy(
                src_ref=piece.at[0],
                dst_ref=recv.at[source // 2, :, :half],
                send_sem=c_ss.at[0],
                recv_sem=c_rs.at[source, unit],
                device_id={"seq": me, "tp": sibling},
                device_id_type=MESH,
            )

            @pl.when(jnp.logical_or(g != source, g != slot))
            def _():
                with jax.named_scope(f"arrive{source}_{unit}"):
                    arrival.wait_recv()

    with jax.named_scope("send_waits"):
        for copy in started + w_copies + pair_copies:
            copy.wait_send()
        for order, copy in c_copies:
            if order > 0:
                copy.wait_send()

        @pl.when(g != slot)
        def _():
            for order, copy in c_copies:
                if order == 0:
                    copy.wait_send()

        @pl.when(inner == 0)
        def _():
            second_queries.wait_send()

        @pl.when(inner == 1)
        def _():
            for copy in query_forwards:
                copy.wait_send()


def add_kernel(pieces, out_hbm, result, sems):
    bands = sems.shape[0]
    rows = result.shape[0] // bands
    copies = []
    for band in range(bands):
        where = slice(band * rows, (band + 1) * rows)
        total = pieces[0, where].astype(jnp.float32)
        for part in range(1, pieces.shape[0]):
            total = total + pieces[part, where].astype(jnp.float32)
        result[where] = total.astype(result.dtype)
        copy = pltpu.make_async_copy(result.at[where], out_hbm.at[where], sems.at[band])
        copy.start()
        copies.append(copy)
    for copy in copies:
        copy.wait()


def local(queries, keys, values, segment_ids, out_weight):
    rows = queries.shape[0]
    members = lax.axis_size("seq")
    slots = lax.axis_size("tp")
    per = members // slots
    heads = queries.shape[1] // HEAD_DIM
    out_width = out_weight.shape[1] * per
    units = out_width // 512 if out_weight.shape[1] % 512 == 0 else 1
    half = out_width // units // 2
    chunk_count = 16
    tiles = members // 2
    group = heads
    while group > 1 and tiles * group * rows * 2 * rows * 4 > 20 * 1024 * 1024:
        group //= 2
    exponent = np.arange(HEAD_DIM // 2, dtype=np.float32) * np.float32(2.0 / HEAD_DIM)
    inverse = np.power(np.float32(rope_base), -exponent).astype(np.float32)
    inverse = jnp.asarray(np.concatenate([inverse, inverse])[None, :])
    vmem = pl.BlockSpec(memory_space=pltpu.VMEM)
    bf16, f32 = jnp.bfloat16, jnp.float32
    dma = pltpu.SemaphoreType.DMA
    buffers = [
        pltpu.VMEM((1, HEAD_DIM), f32),
        pltpu.VMEM(queries.shape, bf16),
        pltpu.VMEM(keys.shape, bf16),
        pltpu.VMEM((members, 1, rows), jnp.int32),
        pltpu.VMEM((tiles, 2 * rows, HEAD_DIM), bf16),
        pltpu.VMEM((tiles, 2 * rows, HEAD_DIM), bf16),
        pltpu.VMEM((slots, rows, queries.shape[1]), bf16),
        pltpu.VMEM((out_weight.shape[0], out_width), bf16),
        pltpu.VMEM((slots, rows, queries.shape[1]), bf16),
        pltpu.VMEM((group, rows, HEAD_DIM), f32),
        pltpu.VMEM((group, rows, HEAD_DIM), f32),
        pltpu.VMEM((group, rows, HEAD_DIM), f32),
        pltpu.VMEM((tiles, group, rows, 2 * rows), f32),
        pltpu.VMEM((slots * units, rows, half), bf16),
        pltpu.VMEM((slots * units, rows, half), bf16),
        pltpu.VMEM((2, rows, half), f32),
        pltpu.VMEM((slots * units, rows, half), bf16),
    ]
    semaphores = [dma((5,))]
    semaphores += [dma((members - 1,))] * 2
    semaphores += [dma((slots - 1,))] * 4
    semaphores += [dma((slots * (per - 1),))] * 4
    semaphores += [dma((slots,))] * 2
    semaphores += [dma((chunk_count * (per - 1),))] * 2
    semaphores += [dma(()), pltpu.SemaphoreType.REGULAR]
    semaphores += [dma((slots * units,))] * 3
    semaphores += [dma((slots, units))]
    on_chip = sum(math.prod(item.shape) * jnp.dtype(item.dtype).itemsize for item in buffers)
    operands = (inverse, queries, keys, values, segment_ids.reshape(1, rows), out_weight)
    pieces = pl.pallas_call(
        functools.partial(layer_kernel, members, slots),
        out_shape=jax.ShapeDtypeStruct((slots // 2, rows, out_width), bf16),
        in_specs=[pl.BlockSpec(memory_space=pl.ANY)] * 6,
        out_specs=vmem,
        scratch_shapes=buffers + semaphores,
        compiler_params=pltpu.CompilerParams(
            collective_id=0, has_side_effects=True, vmem_limit_bytes=on_chip + 8 * 1024 * 1024
        ),
    )(*[pltpu.with_memory_space_constraint(x, pltpu.HBM) for x in operands])
    return pl.pallas_call(
        add_kernel,
        out_shape=jax.ShapeDtypeStruct((rows, out_width), bf16),
        in_specs=[vmem],
        out_specs=pl.BlockSpec(memory_space=pl.ANY),
        scratch_shapes=[pltpu.VMEM((rows, out_width), bf16), dma((4,))],
        compiler_params=pltpu.CompilerParams(vmem_limit_bytes=4 * 1024 * 1024),
    )(pieces)


def solution(mesh):
    return jax.shard_map(
        local,
        mesh=mesh,
        in_specs=(P("seq", "tp"), P("seq", "tp"), P("seq", "tp"), P("seq"), P("tp", "seq")),
        out_specs=P("seq", "tp"),
        check_vma=False,
    )
```

```python
import functools
import math

import jax
import jax.numpy as jnp
import numpy as np
from jax import lax
from jax.experimental import pallas as pl
from jax.experimental.pallas import tpu as pltpu
from jax.sharding import PartitionSpec as P

HEADS = 32
KV_HEADS = 4
HEAD_DIM = 128
SEGMENTS = 16

rope_base = 500000.0
masked_score = -1e30
MESH = pl.DeviceIdType.MESH


def to_column(row_values, count):
    down = lax.broadcasted_iota(jnp.int32, (count, count), 0)
    across = lax.broadcasted_iota(jnp.int32, (count, count), 1)
    return jnp.sum(jnp.where(down == across, row_values, 0.0), axis=1, keepdims=True)


def doc_start_column(seg_all, block, members, rows):
    own = to_column(seg_all[block].astype(jnp.float32), rows)
    earlier = jnp.zeros((rows, rows), jnp.float32)
    for member in range(members):
        earlier = earlier + jnp.where(seg_all[member].astype(jnp.float32) < own, 1.0, 0.0)
    return jnp.sum(earlier, axis=1, keepdims=True)


def layer_kernel(
    members, slots, cuts, own_cuts, chunk_count, inverse_hbm, q_hbm, k_hbm, v_hbm, seg_hbm, w_hbm, recv,
    inverse_ref, q_ref, k_ref, seg_all, k_all, v_all, q_all, w_all, attended,
    top, total, acc, scores_ref, starts_ref, half_send, half_recv, half_own, piece, in_sems,
    seg_ss, seg_rs, k_ss, k_rs, v_ss, v_rs, k2_ss, k2_rs, v2_ss, v2_rs, q_ss, q_rs,
    w_ss, w_rs, own_sem, clear, d_ss, d_rs, c_ss, c_rs,
):
    rows = q_ref.shape[0]
    heads = q_ref.shape[1] // HEAD_DIM
    width = w_hbm.shape[1]
    out_width = recv.shape[2]
    tp_count = slots
    per = members // slots
    me = lax.axis_index("seq")
    g = lax.axis_index("tp")
    slot = lax.div(me, per)
    place = lax.rem(me, per)
    core = lax.rem(g, 2)
    sibling = g + 1 - 2 * core
    assert slots == 4 and q_ref.shape[1] == out_width // 2

    def part_of(ref, block):
        return ref.at[
            lax.div(block, 2), pl.ds(pl.multiple_of(lax.rem(block, 2) * rows, rows), rows)
        ]

    inputs = [
        (seg_hbm, seg_all.at[me]),
        (v_hbm, part_of(v_all, me)),
        (k_hbm, k_ref),
        (inverse_hbm, inverse_ref),
        (q_hbm, q_ref),
    ]
    inputs = [
        pltpu.make_async_copy(source, target, in_sems.at[i])
        for i, (source, target) in enumerate(inputs)
    ]
    for copy in inputs:
        copy.start()

    barrier = pltpu.get_barrier_semaphore()
    for d in range(1, members):
        pl.semaphore_signal(
            barrier, inc=1, device_id={"seq": lax.rem(me + d, members)}, device_id_type=MESH
        )
    for e in range(1, tp_count):
        for d in range(slots):
            pl.semaphore_signal(
                barrier,
                inc=1,
                device_id={
                    "seq": lax.rem(slot + d, slots) * per + place,
                    "tp": lax.rem(g + e, tp_count),
                },
                device_id_type=MESH,
            )

    own_columns = pl.ds(pl.multiple_of(place * width, width), width)
    own_weight = pltpu.make_async_copy(w_hbm, w_all.at[:, own_columns], own_sem)
    own_weight.start()
    for copy in inputs:
        copy.wait()

    with jax.named_scope("barrier_wait"):
        pl.semaphore_wait(barrier, members - 1 + (tp_count - 1) * slots)

    def send(source, target, send_sem, recv_sem, peer):
        return pltpu.make_async_remote_copy(
            src_ref=source,
            dst_ref=target,
            send_sem=send_sem,
            recv_sem=recv_sem,
            device_id={"seq": peer},
            device_id_type=MESH,
        )

    def from_slot(d):
        return lax.rem(slot + slots - d, slots) * per + place

    def to_slots(source, target, ss, rs):
        return [
            send(source, target, ss.at[d - 1], rs.at[d - 1], lax.rem(slot + d, slots) * per + place)
            for d in range(1, slots)
        ]

    def relay(ref, d, ss, rs):
        block = from_slot(d)
        return [
            send(
                part_of(ref, block),
                part_of(ref, block),
                ss.at[d * (per - 1) + r - 1],
                rs.at[d * (per - 1) + r - 1],
                slot * per + lax.rem(place + r, per),
            )
            for r in range(1, per)
        ]

    def start_all(copies):
        for copy in copies:
            copy.start()
        return copies

    started = []
    seg_copies = start_all(
        [
            send(seg_all.at[me], seg_all.at[me], seg_ss, seg_rs, lax.rem(me + d, members))
            for d in range(1, members)
        ]
    )

    def all_of(ref, send_sem, recv_sem):
        return send(ref, ref, send_sem, recv_sem, me)

    all_segs = all_of(seg_all.at[pl.ds(0, members - 1)], seg_ss, seg_rs)
    v_own = part_of(v_all, me)
    v_copies = start_all(to_slots(v_own, v_own, v_ss, v_rs))
    started += v_copies
    v_relays = start_all(relay(v_all, 0, v2_ss, v2_rs))

    units = []
    if len(cuts) > 1:
        for r in range(per):
            for first, size in cuts if r else own_cuts:
                units.append((lax.rem(place + r, per) * width + first, size, r))
    else:
        units.append((0, out_width, None))
    w_copies, w_arrivals = [], {}
    for cut, (first, size) in enumerate(cuts):
        bands = chunk_count * size // width
        band_rows = w_hbm.shape[0] // bands
        for c in range(bands):
            band = pl.ds(c * band_rows, band_rows)
            target_columns = pl.ds(pl.multiple_of(place * width + first, size), size)
            for r in range(1, per):
                copy = send(
                    w_hbm.at[band, first : first + size],
                    w_all.at[band, target_columns],
                    w_ss.at[r - 1],
                    w_rs.at[cut, r - 1],
                    slot * per + lax.rem(place + r, per),
                )
                w_copies.append(copy)
        for r in range(1, per):
            w_arrivals[per - r, first] = all_of(w_all.at[:, :size], w_ss.at[0], w_rs.at[cut, r - 1])
    early = per - 1
    start_all(w_copies[:early])

    with jax.named_scope("seg_wait"):
        all_segs.wait_recv()

    row_index = lax.broadcasted_iota(jnp.int32, (rows, 1), 0)
    position = (me * rows + row_index).astype(jnp.float32) - doc_start_column(
        seg_all, me, members, rows
    )
    angle = position * inverse_ref[...]
    cosine = jnp.cos(angle)
    lane = lax.broadcasted_iota(jnp.int32, (rows, HEAD_DIM), 1)
    sine = jnp.where(lane < HEAD_DIM // 2, -1.0, 1.0) * jnp.sin(angle)

    def rotated(values):
        wide = values.astype(jnp.float32)
        return (wide * cosine + pltpu.roll(wide, HEAD_DIM // 2, 1) * sine).astype(jnp.bfloat16)

    k_own = part_of(k_all, me)
    k_own[...] = rotated(k_ref[...])
    k_copies = start_all(to_slots(k_own, k_own, k_ss, k_rs))
    started += k_copies
    k_relays = start_all(relay(k_all, 0, k2_ss, k2_rs))

    for head in range(heads):
        lanes = slice(head * HEAD_DIM, (head + 1) * HEAD_DIM)
        q_all[slot, :, lanes] = rotated(q_ref[:, lanes])
    pair = slot + 1 - 2 * lax.rem(slot, 2)
    inner = lax.rem(lax.div(slot + 1, 2), 2)
    third = 2 - lax.div(slot, 2)
    fourth = (slots - 1) * (1 - lax.div(slot, 2))

    def send_queries(block_slot, target_slot, index):
        return send(
            q_all.at[block_slot],
            q_all.at[block_slot],
            q_ss.at[index],
            q_rs.at[block_slot],
            target_slot * per + place,
        )

    first_queries, second_queries = send_queries(slot, pair, 0), send_queries(slot, third, 1)
    first_queries.start()
    started.append(first_queries)

    @pl.when(inner == 1)
    def _():
        second_queries.start()


    for other in range(slots):
        starts_ref[other] = jnp.broadcast_to(
            doc_start_column(seg_all, other * per + place, members, rows), (rows, HEAD_DIM)
        ).astype(jnp.int32)

    for d in range(1, slots):
        with jax.named_scope(f"v_wait{d}"):
            v_copies[d - 1].wait_recv()
        v_relays += start_all(relay(v_all, d, v2_ss, v2_rs))
    for d in range(1, slots):
        with jax.named_scope(f"k_wait{d}"):
            k_copies[d - 1].wait_recv()
        k_relays += start_all(relay(k_all, d, k2_ss, k2_rs))
    started += v_relays + k_relays
    start_all(w_copies[early:])
    with jax.named_scope("kv_relay_wait"):
        for copy in v_relays + k_relays:
            copy.wait_recv()

    tile_rows = k_all.shape[1]
    reach = -(-(3 * members * rows // 4 - 1) // rows)
    score_scale = math.log2(math.e) / math.sqrt(HEAD_DIM)

    group = scores_ref.shape[1]

    def attend(block_slot):
        block = block_slot * per + place
        start = starts_ref[block_slot]
        query_index = block * rows + lax.broadcasted_iota(jnp.int32, (rows, tile_rows), 0)
        first = lax.div(jnp.maximum(block - reach, 0), 2)
        last = lax.div(block, 2) + 1
        parts = [slice(p * HEAD_DIM, (p + 1) * HEAD_DIM) for p in range(tile_rows // HEAD_DIM)]
        for base in range(0, heads, group):
            top[...] = jnp.full(top.shape, masked_score, jnp.float32)
            total[...] = jnp.zeros(total.shape, jnp.float32)
            acc[...] = jnp.zeros(acc.shape, jnp.float32)

            def score_tile(number, unused):
                key_index = number * tile_rows + lax.broadcasted_iota(
                    jnp.int32, (rows, tile_rows), 1
                )
                visible = (key_index <= query_index) & (
                    key_index >= jnp.concatenate([start] * len(parts), axis=1)
                )
                bias = jnp.where(visible, 0.0, masked_score)
                key_tile = k_all[number]
                for head in range(group):
                    lanes = slice((base + head) * HEAD_DIM, (base + head + 1) * HEAD_DIM)
                    scores = lax.dot_general(
                        q_all[block_slot, :, lanes],
                        key_tile,
                        (((1,), (1,)), ((), ())),
                        preferred_element_type=jnp.float32,
                    )
                    scores = scores * score_scale + bias
                    scores_ref[number, head] = scores
                    best = top[head]
                    for part in parts:
                        best = jnp.maximum(best, scores[:, part])
                    top[head] = best
                return unused

            lax.fori_loop(first, last, score_tile, 0)
            for head in range(group):
                top[head] = jnp.broadcast_to(
                    jnp.max(top[head], axis=1, keepdims=True), (rows, HEAD_DIM)
                )

            def value_tile(number, unused):
                values = v_all[number]
                for head in range(group):
                    weights = jnp.exp2(
                        scores_ref[number, head] - jnp.concatenate([top[head]] * len(parts), axis=1)
                    )
                    added = total[head]
                    for part in parts:
                        added = added + weights[:, part]
                    total[head] = added
                    acc[head] = acc[head] + jnp.dot(
                        weights.astype(jnp.bfloat16), values, preferred_element_type=jnp.float32
                    )
                return unused

            lax.fori_loop(first, last, value_tile, 0)
            for head in range(group):
                lanes = slice((base + head) * HEAD_DIM, (base + head + 1) * HEAD_DIM)
                attended[block_slot, :, lanes] = (
                    acc[head] / jnp.sum(total[head], axis=1, keepdims=True)
                ).astype(jnp.bfloat16)

    y_index = lax.div(g, 2)

    def across_copy(unit, block_slot, index, half):
        where = unit if block_slot is None else (unit, block_slot)
        where = (where, slice(None), slice(None), slice(half)) if block_slot is None else (
            *where, slice(None), slice(half)
        )
        return pltpu.make_async_remote_copy(
            src_ref=half_send.at[where],
            dst_ref=half_recv.at[where],
            send_sem=d_ss,
            recv_sem=d_rs.at[index],
            device_id={"tp": sibling},
            device_id_type=MESH,
        )

    def multiply(block_slot, unit, given):
        start, size, _ = units[unit]
        half = size // 2
        step = min(256, half)
        first = start + (1 - core if given else core) * half
        if block_slot is None:
            left = attended[...].reshape(slots * rows, attended.shape[2])
        else:
            left = attended[block_slot]
        for c in range(half // step):
            lanes = slice(c * step, (c + 1) * step)
            product = jnp.dot(
                left,
                w_all[:, pl.ds(pl.multiple_of(first + c * step, step), step)],
                preferred_element_type=jnp.float32,
            )
            if block_slot is None:
                product = product.reshape(slots, rows, step)
                where = (unit, slice(None), slice(None), lanes)
            else:
                where = (unit, block_slot, slice(None), lanes)
            if given:
                half_send[where] = product.astype(jnp.bfloat16)
            else:
                half_own[where[1:]] = product

    def exchange(block_slot, unit, index):
        copy = across_copy(unit, block_slot, index, units[unit][1] // 2)
        copy.start()
        return copy

    def finish(block_slot, unit, order):
        start, size, _ = units[unit]
        half = size // 2
        kept = start + core * half
        lanes = slice(half)
        index = order * len(units) + unit
        piece[index, :, lanes] = (
            half_own[block_slot, :, lanes]
            + half_recv[unit, block_slot, :, lanes].astype(jnp.float32)
        ).astype(jnp.bfloat16)
        source = piece.at[index, :, lanes]
        target = recv.at[y_index, :, pl.ds(pl.multiple_of(kept, half), half)]
        copy = pltpu.make_async_remote_copy(
            src_ref=source,
            dst_ref=target,
            send_sem=c_ss.at[min(order, 1)],
            recv_sem=c_rs.at[g],
            device_id={"seq": block_slot * per + place, "tp": slot},
            device_id_type=MESH,
        )
        if order == 0:

            @pl.when(g == slot)
            def _():
                target[...] = source[...]

            @pl.when(g != slot)
            def _():
                copy.start()
        else:
            copy.start()

    def pass_on(block_slot, index):
        copy = send_queries(block_slot, pair, index)

        @pl.when(inner == 1)
        def _():
            with jax.named_scope(f"forward_wait{index}"):
                copy.wait_recv()
            copy.start()

        return copy

    def own_products(block_slot, order):
        if len(units) > 1:
            with jax.named_scope(f"product{order}"):
                copies = []
                for unit in range(len(own_cuts)):
                    multiply(block_slot, unit, True)
                    copies.append(exchange(block_slot, unit, unit * slots + order))
                for unit in range(len(own_cuts)):
                    multiply(block_slot, unit, False)
                    with jax.named_scope(f"across_wait{unit}_{order}"):
                        copies[unit].wait_recv()
                    finish(block_slot, unit, order)

    second_block = pair + inner * (third - pair)
    third_block = third + inner * (fourth - third)
    fourth_block = fourth + inner * (pair - fourth)
    query_forwards = []

    def wait_queries(block_slot, only_outer=False):
        arrived = send_queries(block_slot, pair, 0)
        if only_outer:

            @pl.when(inner == 0)
            def _():
                with jax.named_scope("q_wait_outer"):
                    arrived.wait_recv()
        else:
            with jax.named_scope("q_wait_last"):
                arrived.wait_recv()

    with jax.named_scope("attend0"):
        attend(slot)

    @pl.when(inner == 1)
    def _():
        with jax.named_scope("second_q_sent"):
            second_queries.wait_send()
        pl.semaphore_signal(
            clear, inc=1, device_id={"seq": pair * per + place}, device_id_type=MESH
        )

    @pl.when(inner == 0)
    def _():
        with jax.named_scope("clear_wait"):
            pl.semaphore_wait(clear, 1)
        second_queries.start()

    query_forwards.append(pass_on(third, 2))
    wait_queries(pair, only_outer=True)
    with jax.named_scope("attend1"):
        attend(second_block)
    own_weight.wait()
    own_products(second_block, 1)
    own_products(slot, 0)
    query_forwards.append(pass_on(fourth, 3))
    wait_queries(third, only_outer=True)
    with jax.named_scope("attend2"):
        attend(third_block)
    own_products(third_block, 2)
    wait_queries(fourth_block)
    with jax.named_scope("attend3"):
        attend(fourth_block)
    own_products(fourth_block, 3)

    for unit in range(len(own_cuts) if len(units) > 1 else 0, len(units)):
        start, size, sender = units[unit]
        with jax.named_scope(f"w_wait{unit}"):
            if sender is None:
                for copy in w_arrivals.values():
                    copy.wait_recv()
            else:
                w_arrivals[sender, cuts[(unit - len(own_cuts)) % len(cuts)][0]].wait_recv()
        multiply(None, unit, True)
        copy = exchange(None, unit, len(own_cuts) * slots + unit)
        multiply(None, unit, False)
        with jax.named_scope(f"across_wait{unit}"):
            copy.wait_recv()
        for order, block_slot in ((3, fourth), (2, third), (1, pair), (0, slot)):
            finish(block_slot, unit, order)

    for source in range(tp_count):
        arrival = all_of(recv.at[source // 2, :, : out_width // 2], c_ss.at[0], c_rs.at[source])

        @pl.when(jnp.logical_or(g != source, g != slot))
        def _():
            with jax.named_scope(f"arrive{source}"):
                arrival.wait_recv()

    with jax.named_scope("send_waits"):
        all_segs.wait_send()
        for copy in started:
            copy.wait_send()
        for r in range(1, per):
            all_of(w_all.at[:, :width], w_ss.at[r - 1], w_rs.at[0, 0]).wait_send()
        all_of(attended, d_ss, d_rs.at[0]).wait_send()
        all_of(attended.at[pl.ds(0, slots - 1)], c_ss.at[1], c_rs.at[0]).wait_send()

        @pl.when(g != slot)
        def _():
            all_of(attended.at[0], c_ss.at[0], c_rs.at[0]).wait_send()

        @pl.when(inner == 0)
        def _():
            second_queries.wait_send()

        @pl.when(inner == 1)
        def _():
            for copy in query_forwards:
                copy.wait_send()


def add_kernel(pieces, out_hbm, result, sems):
    bands = sems.shape[0]
    rows = result.shape[0] // bands
    copies = []
    for band in range(bands):
        where = slice(band * rows, (band + 1) * rows)
        total = pieces[0, where].astype(jnp.float32)
        for part in range(1, pieces.shape[0]):
            total = total + pieces[part, where].astype(jnp.float32)
        result[where] = total.astype(result.dtype)
        copy = pltpu.make_async_copy(result.at[where], out_hbm.at[where], sems.at[band])
        copy.start()
        copies.append(copy)
    for copy in copies:
        copy.wait()


def local(queries, keys, values, segment_ids, out_weight):
    rows = queries.shape[0]
    members = lax.axis_size("seq")
    slots = lax.axis_size("tp")
    per = members // slots
    heads = queries.shape[1] // HEAD_DIM
    out_width = out_weight.shape[1] * per
    width = out_weight.shape[1]
    if width % 1024 == 0:
        own_cuts = [(0, width // 2), (width // 2, width // 2)]
        cuts = [(0, width // 2), (width // 2, width // 4), (3 * width // 4, width // 4)]
        units = len(own_cuts) + (per - 1) * len(cuts)
        half = width // 4
    else:
        own_cuts = cuts = [(0, width)]
        units = 1
        half = out_width // 2
    chunk_count = 16
    tiles = members // 2
    group = heads
    while group > 1 and tiles * group * rows * 2 * rows * 4 > 20 * 1024 * 1024:
        group //= 2
    exponent = np.arange(HEAD_DIM // 2, dtype=np.float32) * np.float32(2.0 / HEAD_DIM)
    inverse = np.power(np.float32(rope_base), -exponent).astype(np.float32)
    inverse = jnp.asarray(np.concatenate([inverse, inverse])[None, :])
    vmem = pl.BlockSpec(memory_space=pltpu.VMEM)
    bf16, f32 = jnp.bfloat16, jnp.float32
    dma = pltpu.SemaphoreType.DMA
    buffers = [
        pltpu.VMEM((1, HEAD_DIM), f32),
        pltpu.VMEM(queries.shape, bf16),
        pltpu.VMEM(keys.shape, bf16),
        pltpu.VMEM((members, 1, rows), jnp.int32),
        pltpu.VMEM((tiles, 2 * rows, HEAD_DIM), bf16),
        pltpu.VMEM((tiles, 2 * rows, HEAD_DIM), bf16),
        pltpu.VMEM((slots, rows, queries.shape[1]), bf16),
        pltpu.VMEM((out_weight.shape[0], out_width), bf16),
        pltpu.VMEM((slots, rows, queries.shape[1]), bf16),
        pltpu.VMEM((group, rows, HEAD_DIM), f32),
        pltpu.VMEM((group, rows, HEAD_DIM), f32),
        pltpu.VMEM((group, rows, HEAD_DIM), f32),
        pltpu.VMEM((tiles, group, rows, 2 * rows), f32),
        pltpu.VMEM((slots, rows, HEAD_DIM), jnp.int32),
        pltpu.VMEM((units, slots, rows, half), bf16),
        pltpu.VMEM((units, slots, rows, half), bf16),
        pltpu.VMEM((slots, rows, half), f32),
        pltpu.VMEM((slots * units, rows, half), bf16),
    ]
    semaphores = [dma((5,))]
    semaphores += [dma(())] * 2
    semaphores += [dma((slots - 1,))] * 4
    semaphores += [dma((slots * (per - 1),))] * 4
    semaphores += [dma((slots,))] * 2
    semaphores += [dma((per - 1,)), dma((len(cuts), per - 1))]
    semaphores += [dma(()), pltpu.SemaphoreType.REGULAR]
    semaphores += [dma(()), dma((len(own_cuts) * slots + units,)), dma((2,))]
    semaphores += [dma((slots,))]
    on_chip = sum(math.prod(item.shape) * jnp.dtype(item.dtype).itemsize for item in buffers)
    operands = (inverse, queries, keys, values, segment_ids.reshape(1, rows), out_weight)
    pieces = pl.pallas_call(
        functools.partial(layer_kernel, members, slots, cuts, own_cuts, chunk_count),
        out_shape=pltpu.VMEM((slots // 2, rows, out_width), bf16),
        in_specs=[pl.BlockSpec(memory_space=pl.ANY)] * 6,
        out_specs=pl.BlockSpec(memory_space=pltpu.VMEM),
        scratch_shapes=buffers + semaphores,
        compiler_params=pltpu.CompilerParams(
            collective_id=0, has_side_effects=True, vmem_limit_bytes=on_chip + 8 * 1024 * 1024
        ),
    )(*[pltpu.with_memory_space_constraint(x, pltpu.HBM) for x in operands])
    return pl.pallas_call(
        add_kernel,
        out_shape=jax.ShapeDtypeStruct((rows, out_width), bf16),
        in_specs=[vmem],
        out_specs=pl.BlockSpec(memory_space=pl.ANY),
        scratch_shapes=[pltpu.VMEM((rows, out_width), bf16), dma((4,))],
        compiler_params=pltpu.CompilerParams(vmem_limit_bytes=4 * 1024 * 1024),
    )(pieces)


def solution(mesh):
    return jax.shard_map(
        local,
        mesh=mesh,
        in_specs=(P("seq", "tp"), P("seq", "tp"), P("seq", "tp"), P("seq"), P("tp", "seq")),
        out_specs=P("seq", "tp"),
        check_vma=False,
    )
```

```python
import functools
import math

import jax
import jax.numpy as jnp
import numpy as np
from jax import lax
from jax.experimental import pallas as pl
from jax.experimental.pallas import tpu as pltpu
from jax.sharding import PartitionSpec as P

HEADS = 32
KV_HEADS = 4
HEAD_DIM = 128
SEGMENTS = 16

rope_base = 500000.0
masked_score = -1e30
MESH = pl.DeviceIdType.MESH


def to_column(row_values, count):
    down = lax.broadcasted_iota(jnp.int32, (count, count), 0)
    across = lax.broadcasted_iota(jnp.int32, (count, count), 1)
    return jnp.sum(jnp.where(down == across, row_values, 0.0), axis=1, keepdims=True)


def doc_start_column(seg_all, block, members, rows):
    own = to_column(seg_all[block].astype(jnp.float32), rows)
    earlier = jnp.zeros((rows, rows), jnp.float32)
    for member in range(members):
        earlier = earlier + jnp.where(seg_all[member].astype(jnp.float32) < own, 1.0, 0.0)
    return jnp.sum(earlier, axis=1, keepdims=True)


def layer_kernel(
    members, slots, cuts, own_cuts, solo, chunk_count, inverse_hbm, q_hbm, k_hbm, v_hbm, seg_hbm, w_hbm, recv,
    inverse_ref, q_ref, k_ref, seg_all, k_all, v_all, q_all, w_all, attended,
    top, total, acc, scores_ref, starts_ref, half_send, half_recv, half_own, piece, in_sems,
    seg_ss, seg_rs, k_ss, k_rs, v_ss, v_rs, k2_ss, k2_rs, v2_ss, v2_rs, q_ss, q_rs,
    w_ss, w_rs, own_sem, clear, d_ss, d_rs, c_ss, c_rs,
):
    rows = q_ref.shape[0]
    heads = q_ref.shape[1] // HEAD_DIM
    width = w_hbm.shape[1]
    out_width = recv.shape[2]
    tp_count = slots
    per = members // slots
    me = lax.axis_index("seq")
    g = lax.axis_index("tp")
    slot = lax.div(me, per)
    place = lax.rem(me, per)
    core = lax.rem(g, 2)
    sibling = g + 1 - 2 * core
    assert slots == 4 and q_ref.shape[1] == out_width // 2

    def part_of(ref, block):
        return ref.at[
            lax.div(block, 2), pl.ds(pl.multiple_of(lax.rem(block, 2) * rows, rows), rows)
        ]

    inputs = [
        (seg_hbm, seg_all.at[me]),
        (v_hbm, part_of(v_all, me)),
        (k_hbm, k_ref),
        (inverse_hbm, inverse_ref),
        (q_hbm, q_ref),
    ]
    inputs = [
        pltpu.make_async_copy(source, target, in_sems.at[i])
        for i, (source, target) in enumerate(inputs)
    ]
    for copy in inputs:
        copy.start()

    barrier = pltpu.get_barrier_semaphore()
    for d in range(1, members):
        pl.semaphore_signal(
            barrier, inc=1, device_id={"seq": lax.rem(me + d, members)}, device_id_type=MESH
        )
    for e in range(1, tp_count):
        for d in range(slots):
            pl.semaphore_signal(
                barrier,
                inc=1,
                device_id={
                    "seq": lax.rem(slot + d, slots) * per + place,
                    "tp": lax.rem(g + e, tp_count),
                },
                device_id_type=MESH,
            )

    own_columns = pl.ds(pl.multiple_of(place * width, width), width)
    own_weight = pltpu.make_async_copy(w_hbm, w_all.at[:, own_columns], own_sem)
    own_weight.start()
    for copy in inputs:
        copy.wait()

    with jax.named_scope("barrier_wait"):
        pl.semaphore_wait(barrier, members - 1 + (tp_count - 1) * slots)

    def send(source, target, send_sem, recv_sem, peer):
        return pltpu.make_async_remote_copy(
            src_ref=source,
            dst_ref=target,
            send_sem=send_sem,
            recv_sem=recv_sem,
            device_id={"seq": peer},
            device_id_type=MESH,
        )

    def from_slot(d):
        return lax.rem(slot + slots - d, slots) * per + place

    def to_slots(source, target, ss, rs):
        return [
            send(source, target, ss.at[d - 1], rs.at[d - 1], lax.rem(slot + d, slots) * per + place)
            for d in range(1, slots)
        ]

    def relay(ref, block, index, ss, rs):
        return [
            send(
                part_of(ref, block),
                part_of(ref, block),
                ss.at[index * (per - 1) + r - 1],
                rs.at[index * (per - 1) + r - 1],
                slot * per + lax.rem(place + r, per),
            )
            for r in range(1, per)
        ]

    pair = slot + 1 - 2 * lax.rem(slot, 2)
    inner = lax.rem(lax.div(slot + 1, 2), 2)
    third = 2 - lax.div(slot, 2)
    fourth = (slots - 1) * (1 - lax.div(slot, 2))

    def send_keys(source, target_slot, send_sem):
        block = part_of(k_all, source * per + place)
        return send(block, block, send_sem, k_rs.at[source], target_slot * per + place)

    def start_all(copies):
        for copy in copies:
            copy.start()
        return copies

    started = []
    seg_copies = start_all(
        [
            send(seg_all.at[me], seg_all.at[me], seg_ss, seg_rs, lax.rem(me + d, members))
            for d in range(1, members)
        ]
    )

    def all_of(ref, send_sem, recv_sem):
        return send(ref, ref, send_sem, recv_sem, me)

    all_segs = all_of(seg_all.at[pl.ds(0, members - 1)], seg_ss, seg_rs)
    v_own = part_of(v_all, me)
    v_copies = start_all(to_slots(v_own, v_own, v_ss, v_rs))
    started += v_copies
    v_relays = start_all(relay(v_all, me, 0, v2_ss, v2_rs))

    units = []
    if len(cuts) > 1:
        for r in range(per):
            for first, size in cuts if r else own_cuts:
                start = lax.rem(place + r, per) * width + first
                units.append((start, size, r, None))
        for u in range(len(units) - solo, len(units)):
            units[u] = (*units[u][:3], u % 2)
    else:
        units.append((0, out_width, None, None))

    def kept_part(unit):
        start, size, _, keeper = units[unit]
        if keeper is not None:
            return start, start, size
        return start + core * (size // 2), start + (1 - core) * (size // 2), size // 2
    w_copies, w_arrivals = [], {}
    for cut, (first, size) in enumerate(cuts):
        bands = chunk_count * size // width
        band_rows = w_hbm.shape[0] // bands
        for c in range(bands):
            band = pl.ds(c * band_rows, band_rows)
            target_columns = pl.ds(pl.multiple_of(place * width + first, size), size)
            for r in range(1, per):
                copy = send(
                    w_hbm.at[band, first : first + size],
                    w_all.at[band, target_columns],
                    w_ss.at[r - 1],
                    w_rs.at[cut, r - 1],
                    slot * per + lax.rem(place + r, per),
                )
                w_copies.append(copy)
        for r in range(1, per):
            w_arrivals[per - r, first] = all_of(w_all.at[:, :size], w_ss.at[0], w_rs.at[cut, r - 1])
    early = per - 1
    start_all(w_copies[:early])

    with jax.named_scope("seg_wait"):
        all_segs.wait_recv()

    row_index = lax.broadcasted_iota(jnp.int32, (rows, 1), 0)
    position = (me * rows + row_index).astype(jnp.float32) - doc_start_column(
        seg_all, me, members, rows
    )
    angle = position * inverse_ref[...]
    cosine = jnp.cos(angle)
    lane = lax.broadcasted_iota(jnp.int32, (rows, HEAD_DIM), 1)
    sine = jnp.where(lane < HEAD_DIM // 2, -1.0, 1.0) * jnp.sin(angle)

    def rotated(values):
        wide = values.astype(jnp.float32)
        return (wide * cosine + pltpu.roll(wide, HEAD_DIM // 2, 1) * sine).astype(jnp.bfloat16)

    k_own = part_of(k_all, me)
    k_own[...] = rotated(k_ref[...])
    started += start_all(
        [send_keys(slot, to, k_ss.at[i]) for i, to in enumerate((pair, third, fourth))]
    )
    k_relays = start_all(relay(k_all, me, 0, k2_ss, k2_rs))

    for head in range(heads):
        lanes = slice(head * HEAD_DIM, (head + 1) * HEAD_DIM)
        q_all[slot, :, lanes] = rotated(q_ref[:, lanes])
    def send_queries(block_slot, target_slot, index):
        return send(
            q_all.at[block_slot],
            q_all.at[block_slot],
            q_ss.at[index],
            q_rs.at[block_slot],
            target_slot * per + place,
        )

    first_queries, second_queries = send_queries(slot, pair, 0), send_queries(slot, third, 1)
    started += start_all([first_queries])

    @pl.when(inner == 1)
    def _():
        second_queries.start()

    for other in range(slots):
        starts_ref[other] = jnp.broadcast_to(
            doc_start_column(seg_all, other * per + place, members, rows), (rows, HEAD_DIM)
        ).astype(jnp.int32)

    for d in range(1, slots):
        with jax.named_scope(f"v_wait{d}"):
            v_copies[d - 1].wait_recv()
        v_relays += start_all(relay(v_all, from_slot(d), d, v2_ss, v2_rs))
    for i, source in enumerate((pair, third, fourth)):
        with jax.named_scope(f"k_wait{i}"):
            send_keys(source, pair, k_ss.at[0]).wait_recv()
        k_relays += start_all(relay(k_all, source * per + place, i + 1, k2_ss, k2_rs))

    started += v_relays + k_relays
    start_all(w_copies[early:])
    with jax.named_scope("kv_relay_wait"):
        for copy in v_relays + k_relays:
            copy.wait_recv()

    tile_rows = k_all.shape[1]
    reach = -(-(3 * members * rows // 4 - 1) // rows)
    score_scale = math.log2(math.e) / math.sqrt(HEAD_DIM)

    group = scores_ref.shape[1]

    def attend(block_slot, between=None):
        block = block_slot * per + place
        start = starts_ref[block_slot]
        query_index = block * rows + lax.broadcasted_iota(jnp.int32, (rows, tile_rows), 0)
        first = lax.div(jnp.maximum(block - reach, 0), 2)
        last = lax.div(block, 2) + 1
        parts = [slice(p * HEAD_DIM, (p + 1) * HEAD_DIM) for p in range(tile_rows // HEAD_DIM)]
        for base in range(0, heads, group):
            top[...] = jnp.full(top.shape, masked_score, jnp.float32)
            total[...] = jnp.zeros(total.shape, jnp.float32)
            acc[...] = jnp.zeros(acc.shape, jnp.float32)

            def score_tile(number, unused):
                key_index = number * tile_rows + lax.broadcasted_iota(
                    jnp.int32, (rows, tile_rows), 1
                )
                visible = (key_index <= query_index) & (
                    key_index >= jnp.concatenate([start] * len(parts), axis=1)
                )
                bias = jnp.where(visible, 0.0, masked_score)
                key_tile = k_all[number]
                for head in range(group):
                    lanes = slice((base + head) * HEAD_DIM, (base + head + 1) * HEAD_DIM)
                    scores = lax.dot_general(
                        q_all[block_slot, :, lanes],
                        key_tile,
                        (((1,), (1,)), ((), ())),
                        preferred_element_type=jnp.float32,
                    )
                    scores = scores * score_scale + bias
                    scores_ref[number, head] = scores
                    best = top[head]
                    for part in parts:
                        best = jnp.maximum(best, scores[:, part])
                    top[head] = best
                return unused

            lax.fori_loop(first, last, score_tile, 0)
            if between is not None and base == 0:
                between()
            for head in range(group):
                top[head] = jnp.broadcast_to(
                    jnp.max(top[head], axis=1, keepdims=True), (rows, HEAD_DIM)
                )

            def value_tile(number, unused):
                values = v_all[number]
                for head in range(group):
                    weights = jnp.exp2(
                        scores_ref[number, head] - jnp.concatenate([top[head]] * len(parts), axis=1)
                    )
                    added = total[head]
                    for part in parts:
                        added = added + weights[:, part]
                    total[head] = added
                    acc[head] = acc[head] + jnp.dot(
                        weights.astype(jnp.bfloat16), values, preferred_element_type=jnp.float32
                    )
                return unused

            lax.fori_loop(first, last, value_tile, 0)
            for head in range(group):
                lanes = slice((base + head) * HEAD_DIM, (base + head + 1) * HEAD_DIM)
                attended[block_slot, :, lanes] = (
                    acc[head] / jnp.sum(total[head], axis=1, keepdims=True)
                ).astype(jnp.bfloat16)

    y_index = lax.div(g, 2)

    def across_copy(unit, block_slot, index, half):
        where = unit if block_slot is None else (unit, block_slot)
        where = (where, slice(None), slice(None), slice(half)) if block_slot is None else (
            *where, slice(None), slice(half)
        )
        return pltpu.make_async_remote_copy(
            src_ref=half_send.at[where],
            dst_ref=half_recv.at[where],
            send_sem=d_ss,
            recv_sem=d_rs.at[index],
            device_id={"tp": sibling},
            device_id_type=MESH,
        )

    def multiply(block_slot, unit, given):
        first, other, half = kept_part(unit)
        first = other if given else first
        step = min(256, half)
        if block_slot is None:
            left = attended[...].reshape(slots * rows, attended.shape[2])
        else:
            left = attended[block_slot]
        for c in range(half // step):
            lanes = slice(c * step, (c + 1) * step)
            product = jnp.dot(
                left,
                w_all[:, pl.ds(pl.multiple_of(first + c * step, step), step)],
                preferred_element_type=jnp.float32,
            )
            if block_slot is None:
                product = product.reshape(slots, rows, step)
                where = (unit, slice(None), slice(None), lanes)
            else:
                where = (unit, block_slot, slice(None), lanes)
            if given:
                half_send[where] = product.astype(jnp.bfloat16)
            else:
                half_own[where[1:]] = product

    def exchange(block_slot, unit, index):
        copy = across_copy(unit, block_slot, index, kept_part(unit)[2])
        copy.start()
        return copy

    def finish(block_slot, unit, order):
        kept, _, half = kept_part(unit)
        lanes = slice(half)
        index = order * len(units) + unit
        piece[index, :, lanes] = (
            half_own[block_slot, :, lanes]
            + half_recv[unit, block_slot, :, lanes].astype(jnp.float32)
        ).astype(jnp.bfloat16)
        source = piece.at[index, :, lanes]
        target = recv.at[y_index, :, pl.ds(pl.multiple_of(kept, half), half)]
        copy = pltpu.make_async_remote_copy(
            src_ref=source,
            dst_ref=target,
            send_sem=c_ss.at[min(order, 1)],
            recv_sem=c_rs.at[g],
            device_id={"seq": block_slot * per + place, "tp": slot},
            device_id_type=MESH,
        )
        if order == 0:

            @pl.when(g == slot)
            def _():
                target[...] = source[...]

            @pl.when(g != slot)
            def _():
                copy.start()
        else:
            copy.start()

    def pass_on(block_slot, index):
        copy = send_queries(block_slot, pair, index)

        @pl.when(inner == 1)
        def _():
            with jax.named_scope(f"forward_wait{index}"):
                copy.wait_recv()
            copy.start()

        return copy

    def own_products(block_slot, order):
        if len(units) > 1:
            with jax.named_scope(f"product{order}"):
                copies = []
                for unit in range(len(own_cuts)):
                    multiply(block_slot, unit, True)
                    copies.append(exchange(block_slot, unit, unit * slots + order))
                for unit in range(len(own_cuts)):
                    multiply(block_slot, unit, False)
                    with jax.named_scope(f"across_wait{unit}_{order}"):
                        copies[unit].wait_recv()
                    finish(block_slot, unit, order)

    second_block = pair + inner * (third - pair)
    third_block = third + inner * (fourth - third)
    fourth_block = fourth + inner * (pair - fourth)
    query_forwards = []

    def wait_queries(block_slot, only_outer=False):
        arrived = send_queries(block_slot, pair, 0)
        if only_outer:

            @pl.when(inner == 0)
            def _():
                with jax.named_scope("q_wait_outer"):
                    arrived.wait_recv()
        else:
            with jax.named_scope("q_wait_last"):
                arrived.wait_recv()

    def release_queries():
        @pl.when(inner == 1)
        def _():
            with jax.named_scope("second_q_sent"):
                second_queries.wait_send()
            pl.semaphore_signal(
                clear, inc=1, device_id={"seq": pair * per + place}, device_id_type=MESH
            )

        @pl.when(inner == 0)
        def _():
            with jax.named_scope("clear_wait"):
                pl.semaphore_wait(clear, 1)
            second_queries.start()

    with jax.named_scope("attend0"):
        attend(slot, release_queries)
    query_forwards.append(pass_on(third, 2))
    wait_queries(pair, only_outer=True)
    with jax.named_scope("attend1"):
        attend(second_block)
    own_weight.wait()
    own_products(second_block, 1)
    own_products(slot, 0)
    query_forwards.append(pass_on(fourth, 3))
    wait_queries(third, only_outer=True)
    with jax.named_scope("attend2"):
        attend(third_block)
    own_products(third_block, 2)
    wait_queries(fourth_block)
    with jax.named_scope("attend3"):
        attend(fourth_block)
    own_products(fourth_block, 3)

    for unit in range(len(own_cuts) if len(units) > 1 else 0, len(units)):
        _, _, sender, keeper = units[unit]
        with jax.named_scope(f"w_wait{unit}"):
            if sender is None:
                for copy in w_arrivals.values():
                    copy.wait_recv()
            else:
                w_arrivals[sender, cuts[(unit - len(own_cuts)) % len(cuts)][0]].wait_recv()
        index = len(own_cuts) * slots + unit

        def give():
            multiply(None, unit, True)
            exchange(None, unit, index)

        def keep():
            multiply(None, unit, False)
            with jax.named_scope(f"across_wait{unit}"):
                across_copy(unit, None, index, kept_part(unit)[2]).wait_recv()
            for order, block_slot in ((3, fourth), (2, third), (1, pair), (0, slot)):
                finish(block_slot, unit, order)

        if keeper is None:
            give()
            keep()
        else:
            pl.when(core == keeper)(keep)
            pl.when(core != keeper)(give)

    for source in range(tp_count):
        arrival = all_of(recv.at[source // 2, :, : out_width // 2], c_ss.at[0], c_rs.at[source])

        @pl.when(jnp.logical_or(g != source, g != slot))
        def _():
            with jax.named_scope(f"arrive{source}"):
                arrival.wait_recv()

    with jax.named_scope("send_waits"):
        all_segs.wait_send()
        for copy in started:
            copy.wait_send()
        for r in range(1, per):
            all_of(w_all.at[:, :width], w_ss.at[r - 1], w_rs.at[0, 0]).wait_send()
        all_of(attended, d_ss, d_rs.at[0]).wait_send()
        all_of(attended.at[pl.ds(0, slots - 1)], c_ss.at[1], c_rs.at[0]).wait_send()

        @pl.when(g != slot)
        def _():
            all_of(attended.at[0], c_ss.at[0], c_rs.at[0]).wait_send()

        @pl.when(inner == 0)
        def _():
            second_queries.wait_send()

        @pl.when(inner == 1)
        def _():
            for copy in query_forwards:
                copy.wait_send()


def add_kernel(pieces, out_hbm, result, sems):
    bands = sems.shape[0]
    rows = result.shape[0] // bands
    copies = []
    for band in range(bands):
        where = slice(band * rows, (band + 1) * rows)
        total = pieces[0, where].astype(jnp.float32)
        for part in range(1, pieces.shape[0]):
            total = total + pieces[part, where].astype(jnp.float32)
        result[where] = total.astype(result.dtype)
        copy = pltpu.make_async_copy(result.at[where], out_hbm.at[where], sems.at[band])
        copy.start()
        copies.append(copy)
    for copy in copies:
        copy.wait()


def local(queries, keys, values, segment_ids, out_weight):
    rows = queries.shape[0]
    members = lax.axis_size("seq")
    slots = lax.axis_size("tp")
    per = members // slots
    heads = queries.shape[1] // HEAD_DIM
    out_width = out_weight.shape[1] * per
    width = out_weight.shape[1]
    if width % 1024 == 0:
        own_cuts = [(0, width // 2), (width // 2, width // 2)]
        cuts = [(0, width // 2), (width // 2, width // 4)]
        cuts += [(3 * width // 4, width // 8), (7 * width // 8, width // 8)]
        solo = 2 if per == 2 else 0
        units = len(own_cuts) + (per - 1) * len(cuts)
        half = width // 4
    else:
        own_cuts = cuts = [(0, width)]
        solo = 0
        units = 1
        half = out_width // 2
    chunk_count = 16
    tiles = members // 2
    group = heads
    while group > 1 and tiles * group * rows * 2 * rows * 4 > 20 * 1024 * 1024:
        group //= 2
    exponent = np.arange(HEAD_DIM // 2, dtype=np.float32) * np.float32(2.0 / HEAD_DIM)
    inverse = np.power(np.float32(rope_base), -exponent).astype(np.float32)
    inverse = jnp.asarray(np.concatenate([inverse, inverse])[None, :])
    vmem = pl.BlockSpec(memory_space=pltpu.VMEM)
    bf16, f32 = jnp.bfloat16, jnp.float32
    dma = pltpu.SemaphoreType.DMA
    buffers = [
        pltpu.VMEM((1, HEAD_DIM), f32),
        pltpu.VMEM(queries.shape, bf16),
        pltpu.VMEM(keys.shape, bf16),
        pltpu.VMEM((members, 1, rows), jnp.int32),
        pltpu.VMEM((tiles, 2 * rows, HEAD_DIM), bf16),
        pltpu.VMEM((tiles, 2 * rows, HEAD_DIM), bf16),
        pltpu.VMEM((slots, rows, queries.shape[1]), bf16),
        pltpu.VMEM((out_weight.shape[0], out_width), bf16),
        pltpu.VMEM((slots, rows, queries.shape[1]), bf16),
        pltpu.VMEM((group, rows, HEAD_DIM), f32),
        pltpu.VMEM((group, rows, HEAD_DIM), f32),
        pltpu.VMEM((group, rows, HEAD_DIM), f32),
        pltpu.VMEM((tiles, group, rows, 2 * rows), f32),
        pltpu.VMEM((slots, rows, HEAD_DIM), jnp.int32),
        pltpu.VMEM((units, slots, rows, half), bf16),
        pltpu.VMEM((units, slots, rows, half), bf16),
        pltpu.VMEM((slots, rows, half), f32),
        pltpu.VMEM((slots * units, rows, half), bf16),
    ]
    semaphores = [dma((5,))]
    semaphores += [dma(())] * 2
    semaphores += [dma((slots - 1,)), dma((slots,))] + [dma((slots - 1,))] * 2
    semaphores += [dma((slots * (per - 1),))] * 4
    semaphores += [dma((slots,))] * 2
    semaphores += [dma((per - 1,)), dma((len(cuts), per - 1))]
    semaphores += [dma(()), pltpu.SemaphoreType.REGULAR]
    semaphores += [dma(()), dma((len(own_cuts) * slots + units,)), dma((2,))]
    semaphores += [dma((slots,))]
    on_chip = sum(math.prod(item.shape) * jnp.dtype(item.dtype).itemsize for item in buffers)
    operands = (inverse, queries, keys, values, segment_ids.reshape(1, rows), out_weight)
    pieces = pl.pallas_call(
        functools.partial(layer_kernel, members, slots, cuts, own_cuts, solo, chunk_count),
        out_shape=pltpu.VMEM((slots // 2, rows, out_width), bf16),
        in_specs=[pl.BlockSpec(memory_space=pl.ANY)] * 6,
        out_specs=pl.BlockSpec(memory_space=pltpu.VMEM),
        scratch_shapes=buffers + semaphores,
        compiler_params=pltpu.CompilerParams(
            collective_id=0, has_side_effects=True, vmem_limit_bytes=on_chip + 8 * 1024 * 1024
        ),
    )(*[pltpu.with_memory_space_constraint(x, pltpu.HBM) for x in operands])
    return pl.pallas_call(
        add_kernel,
        out_shape=jax.ShapeDtypeStruct((rows, out_width), bf16),
        in_specs=[vmem],
        out_specs=pl.BlockSpec(memory_space=pl.ANY),
        scratch_shapes=[pltpu.VMEM((rows, out_width), bf16), dma((4,))],
        compiler_params=pltpu.CompilerParams(vmem_limit_bytes=4 * 1024 * 1024),
    )(pieces)


def solution(mesh):
    return jax.shard_map(
        local,
        mesh=mesh,
        in_specs=(P("seq", "tp"), P("seq", "tp"), P("seq", "tp"), P("seq"), P("tp", "seq")),
        out_specs=P("seq", "tp"),
        check_vma=False,
    )
```

```python
import functools
import math

import jax
import jax.numpy as jnp
import numpy as np
from jax import lax
from jax.experimental import pallas as pl
from jax.experimental.pallas import tpu as pltpu
from jax.sharding import PartitionSpec as P

HEADS = 32
KV_HEADS = 4
HEAD_DIM = 128
SEGMENTS = 16

rope_base = 500000.0
masked_score = -1e30
MESH = pl.DeviceIdType.MESH


def to_column(row_values, count):
    down = lax.broadcasted_iota(jnp.int32, (count, count), 0)
    across = lax.broadcasted_iota(jnp.int32, (count, count), 1)
    return jnp.sum(jnp.where(down == across, row_values, 0.0), axis=1, keepdims=True)


def doc_start_column(seg_all, block, members, rows):
    own = to_column(seg_all[block].astype(jnp.float32), rows)
    earlier = jnp.zeros((rows, rows), jnp.float32)
    for member in range(members):
        earlier = earlier + jnp.where(seg_all[member].astype(jnp.float32) < own, 1.0, 0.0)
    return jnp.sum(earlier, axis=1, keepdims=True)


def layer_kernel(
    members, slots, cuts, own_cuts, solo, chunk_count, inverse_hbm, q_hbm, k_hbm, v_hbm, seg_hbm, w_hbm, recv,
    inverse_ref, q_ref, k_ref, seg_all, k_all, v_all, q_all, w_all, attended,
    top, total, acc, scores_ref, starts_ref, half_send, half_recv, half_own, piece, in_sems,
    seg_ss, seg_rs, kv_ss, k_rs, v_rs, x_ss, x_rs, q_ss, q_rs,
    w_ss, w_rs, own_sem, clear, d_ss, d_rs, c_ss, c_rs,
):
    rows = q_ref.shape[0]
    heads = q_ref.shape[1] // HEAD_DIM
    width = w_hbm.shape[1]
    out_width = recv.shape[2]
    tp_count = slots
    per = members // slots
    me = lax.axis_index("seq")
    g = lax.axis_index("tp")
    slot = lax.div(me, per)
    place = lax.rem(me, per)
    core = lax.rem(g, 2)
    sibling = g + 1 - 2 * core
    assert slots == 4 and q_ref.shape[1] == out_width // 2 == 2 * slots * HEAD_DIM

    def part_of(ref, block):
        return ref.at[
            lax.div(block, 2), pl.ds(pl.multiple_of(lax.rem(block, 2) * rows, rows), rows)
        ]

    inputs = [
        (seg_hbm, seg_all.at[me]),
        (v_hbm, part_of(v_all, me)),
        (k_hbm, k_ref),
        (inverse_hbm, inverse_ref),
        (q_hbm, q_ref),
    ]
    inputs = [
        pltpu.make_async_copy(source, target, in_sems.at[i])
        for i, (source, target) in enumerate(inputs)
    ]
    for copy in inputs:
        copy.start()

    barrier = pltpu.get_barrier_semaphore()
    for d in range(1, members):
        pl.semaphore_signal(
            barrier, inc=1, device_id={"seq": lax.rem(me + d, members)}, device_id_type=MESH
        )
    for e in range(1, tp_count):
        for d in range(slots):
            pl.semaphore_signal(
                barrier,
                inc=1,
                device_id={
                    "seq": lax.rem(slot + d, slots) * per + place,
                    "tp": lax.rem(g + e, tp_count),
                },
                device_id_type=MESH,
            )

    own_columns = pl.ds(pl.multiple_of(place * width, width), width)
    own_weight = pltpu.make_async_copy(w_hbm, w_all.at[:, own_columns], own_sem)
    own_weight.start()
    for copy in inputs:
        copy.wait()

    with jax.named_scope("barrier_wait"):
        pl.semaphore_wait(barrier, members - 1 + (tp_count - 1) * slots)

    def send(source, target, send_sem, recv_sem, peer):
        return pltpu.make_async_remote_copy(
            src_ref=source,
            dst_ref=target,
            send_sem=send_sem,
            recv_sem=recv_sem,
            device_id={"seq": peer},
            device_id_type=MESH,
        )

    def from_slot(d):
        return lax.rem(slot + slots - d, slots) * per + place

    def to_slots(source, target, ss, rs):
        return [
            send(source, target, ss, rs.at[d - 1], lax.rem(slot + d, slots) * per + place)
            for d in range(1, slots)
        ]

    def relay(ref, block, ss, rs):
        return [
            send(
                part_of(ref, block),
                part_of(ref, block),
                ss.at[r - 1],
                rs.at[r - 1],
                slot * per + lax.rem(place + r, per),
            )
            for r in range(1, per)
        ]

    pair = slot + 1 - 2 * lax.rem(slot, 2)
    inner = lax.rem(lax.div(slot + 1, 2), 2)
    third = 2 - lax.div(slot, 2)
    fourth = (slots - 1) * (1 - lax.div(slot, 2))

    def send_keys(source, target_slot, send_sem):
        block = part_of(k_all, source * per + place)
        return send(block, block, send_sem, k_rs.at[source], target_slot * per + place)

    def start_all(copies):
        for copy in copies:
            copy.start()
        return copies

    started = []
    seg_copies = start_all(
        [
            send(seg_all.at[me], seg_all.at[me], seg_ss, seg_rs, lax.rem(me + d, members))
            for d in range(1, members)
        ]
    )

    def all_of(ref, send_sem, recv_sem):
        return send(ref, ref, send_sem, recv_sem, me)

    all_segs = all_of(seg_all.at[pl.ds(0, members - 1)], seg_ss, seg_rs)
    v_own = part_of(v_all, me)
    v_copies = start_all(to_slots(v_own, v_own, kv_ss, v_rs))
    v_relays = start_all(relay(v_all, me, x_ss, x_rs))

    units = []
    if len(cuts) > 1:
        for r in range(per):
            for first, size in cuts if r else own_cuts:
                start = lax.rem(place + r, per) * width + first
                units.append((start, size, r, None))
        for u in range(len(units) - solo, len(units)):
            units[u] = (*units[u][:3], u % 2)
    else:
        units.append((0, out_width, None, None))

    def kept_part(unit):
        start, size, _, keeper = units[unit]
        if keeper is not None:
            return start, start, size
        return start + core * (size // 2), start + (1 - core) * (size // 2), size // 2
    w_copies, w_arrivals = [], {}
    for cut, (first, size) in enumerate(cuts):
        bands = chunk_count * size // width
        band_rows = w_hbm.shape[0] // bands
        for c in range(bands):
            band = pl.ds(c * band_rows, band_rows)
            target_columns = pl.ds(pl.multiple_of(place * width + first, size), size)
            for r in range(1, per):
                copy = send(
                    w_hbm.at[band, first : first + size],
                    w_all.at[band, target_columns],
                    w_ss.at[r - 1],
                    w_rs.at[cut, r - 1],
                    slot * per + lax.rem(place + r, per),
                )
                w_copies.append(copy)
        for r in range(1, per):
            w_arrivals[per - r, first] = all_of(w_all.at[:, :size], w_ss.at[0], w_rs.at[cut, r - 1])
    early = per - 1
    start_all(w_copies[:early])

    with jax.named_scope("seg_wait"):
        all_segs.wait_recv()

    row_index = lax.broadcasted_iota(jnp.int32, (rows, 1), 0)
    position = (me * rows + row_index).astype(jnp.float32) - doc_start_column(
        seg_all, me, members, rows
    )
    angle = position * inverse_ref[...]
    cosine = jnp.cos(angle)
    lane = lax.broadcasted_iota(jnp.int32, (rows, HEAD_DIM), 1)
    sine = jnp.where(lane < HEAD_DIM // 2, -1.0, 1.0) * jnp.sin(angle)

    def rotated(values):
        wide = values.astype(jnp.float32)
        return (wide * cosine + pltpu.roll(wide, HEAD_DIM // 2, 1) * sine).astype(jnp.bfloat16)

    k_own = part_of(k_all, me)
    k_own[...] = rotated(k_ref[...])
    start_all(
        [send_keys(slot, to, kv_ss) for to in (pair, third, fourth)]
    )
    k_relays = start_all(relay(k_all, me, x_ss, x_rs))

    for head in range(heads):
        lanes = slice(head * HEAD_DIM, (head + 1) * HEAD_DIM)
        q_all[slot, :, lanes] = rotated(q_ref[:, lanes])
    def send_queries(block_slot, target_slot, index):
        return send(
            q_all.at[block_slot],
            q_all.at[block_slot],
            q_ss.at[index],
            q_rs.at[block_slot],
            target_slot * per + place,
        )

    first_queries, second_queries = send_queries(slot, pair, 0), send_queries(slot, third, 1)
    started += start_all([first_queries])

    @pl.when(inner == 1)
    def _():
        second_queries.start()

    for other in range(slots):
        starts_ref[other] = jnp.broadcast_to(
            doc_start_column(seg_all, other * per + place, members, rows), (rows, HEAD_DIM)
        ).astype(jnp.int32)

    for d in range(1, slots):
        with jax.named_scope(f"v_wait{d}"):
            v_copies[d - 1].wait_recv()
        v_relays += start_all(relay(v_all, from_slot(d), x_ss, x_rs))
    for i, source in enumerate((pair, third, fourth)):
        with jax.named_scope(f"k_wait{i}"):
            send_keys(source, pair, kv_ss).wait_recv()
        k_relays += start_all(relay(k_all, source * per + place, x_ss, x_rs))

    start_all(w_copies[early:])
    with jax.named_scope("kv_relay_wait"):
        for r in range(1, per):
            all_of(q_ref, x_ss.at[r - 1], x_rs.at[r - 1]).wait_recv()

    tile_rows = k_all.shape[1]
    reach = -(-(3 * members * rows // 4 - 1) // rows)
    score_scale = math.log2(math.e) / math.sqrt(HEAD_DIM)

    group = scores_ref.shape[1]

    def attend(block_slot, between=None):
        block = block_slot * per + place
        start = starts_ref[block_slot]
        query_index = block * rows + lax.broadcasted_iota(jnp.int32, (rows, tile_rows), 0)
        first = lax.div(jnp.maximum(block - reach, 0), 2)
        last = lax.div(block, 2) + 1
        parts = [slice(p * HEAD_DIM, (p + 1) * HEAD_DIM) for p in range(tile_rows // HEAD_DIM)]
        for base in range(0, heads, group):
            top[...] = jnp.full(top.shape, masked_score, jnp.float32)
            total[...] = jnp.zeros(total.shape, jnp.float32)
            acc[...] = jnp.zeros(acc.shape, jnp.float32)

            def score_tile(number, unused):
                key_index = number * tile_rows + lax.broadcasted_iota(
                    jnp.int32, (rows, tile_rows), 1
                )
                visible = (key_index <= query_index) & (
                    key_index >= jnp.concatenate([start] * len(parts), axis=1)
                )
                bias = jnp.where(visible, 0.0, masked_score)
                key_tile = k_all[number]
                for head in range(group):
                    lanes = slice((base + head) * HEAD_DIM, (base + head + 1) * HEAD_DIM)
                    scores = lax.dot_general(
                        q_all[block_slot, :, lanes],
                        key_tile,
                        (((1,), (1,)), ((), ())),
                        preferred_element_type=jnp.float32,
                    )
                    scores = scores * score_scale + bias
                    scores_ref[number, head] = scores
                    best = top[head]
                    for part in parts:
                        best = jnp.maximum(best, scores[:, part])
                    top[head] = best
                return unused

            lax.fori_loop(first, last, score_tile, 0)
            if between is not None and base == 0:
                between()
            for head in range(group):
                top[head] = jnp.broadcast_to(
                    jnp.max(top[head], axis=1, keepdims=True), (rows, HEAD_DIM)
                )

            def value_tile(number, unused):
                values = v_all[number]
                for head in range(group):
                    weights = jnp.exp2(
                        scores_ref[number, head] - jnp.concatenate([top[head]] * len(parts), axis=1)
                    )
                    added = total[head]
                    for part in parts:
                        added = added + weights[:, part]
                    total[head] = added
                    acc[head] = acc[head] + jnp.dot(
                        weights.astype(jnp.bfloat16), values, preferred_element_type=jnp.float32
                    )
                return unused

            lax.fori_loop(first, last, value_tile, 0)
            for head in range(group):
                lanes = slice((base + head) * HEAD_DIM, (base + head + 1) * HEAD_DIM)
                attended[block_slot, :, lanes] = (
                    acc[head] / jnp.sum(total[head], axis=1, keepdims=True)
                ).astype(jnp.bfloat16)

    y_index = lax.div(g, 2)

    def across_copy(unit, block_slot, index, half):
        where = unit if block_slot is None else (unit, block_slot)
        where = (where, slice(None), slice(None), slice(half)) if block_slot is None else (
            *where, slice(None), slice(half)
        )
        return pltpu.make_async_remote_copy(
            src_ref=half_send.at[where],
            dst_ref=half_recv.at[where],
            send_sem=d_ss,
            recv_sem=d_rs.at[index],
            device_id={"tp": sibling},
            device_id_type=MESH,
        )

    def multiply(block_slot, unit, given):
        first, other, half = kept_part(unit)
        first = other if given else first
        step = min(256, half)
        if block_slot is None:
            left = attended[...].reshape(slots * rows, attended.shape[2])
        else:
            left = attended[block_slot]
        for c in range(half // step):
            lanes = slice(c * step, (c + 1) * step)
            product = jnp.dot(
                left,
                w_all[:, pl.ds(pl.multiple_of(first + c * step, step), step)],
                preferred_element_type=jnp.float32,
            )
            if block_slot is None:
                product = product.reshape(slots, rows, step)
                where = (unit, slice(None), slice(None), lanes)
            else:
                where = (unit, block_slot, slice(None), lanes)
            if given:
                half_send[where] = product.astype(jnp.bfloat16)
            else:
                half_own[where[1:]] = product

    def exchange(block_slot, unit, index):
        copy = across_copy(unit, block_slot, index, kept_part(unit)[2])
        copy.start()
        return copy

    def finish(block_slot, unit, order):
        kept, _, half = kept_part(unit)
        lanes = slice(half)
        index = order * len(units) + unit
        piece[index, :, lanes] = (
            half_own[block_slot, :, lanes]
            + half_recv[unit, block_slot, :, lanes].astype(jnp.float32)
        ).astype(jnp.bfloat16)
        source = piece.at[index, :, lanes]
        target = recv.at[y_index, :, pl.ds(pl.multiple_of(kept, half), half)]
        copy = pltpu.make_async_remote_copy(
            src_ref=source,
            dst_ref=target,
            send_sem=c_ss.at[min(order, 1)],
            recv_sem=c_rs.at[g],
            device_id={"seq": block_slot * per + place, "tp": slot},
            device_id_type=MESH,
        )
        if order == 0:

            @pl.when(g == slot)
            def _():
                target[...] = source[...]

            @pl.when(g != slot)
            def _():
                copy.start()
        else:
            copy.start()

    def pass_on(block_slot, index):
        copy = send_queries(block_slot, pair, index)

        @pl.when(inner == 1)
        def _():
            with jax.named_scope(f"forward_wait{index}"):
                copy.wait_recv()
            copy.start()

        return copy

    def own_products(block_slot, order):
        if len(units) > 1:
            with jax.named_scope(f"product{order}"):
                copies = []
                for unit in range(len(own_cuts)):
                    multiply(block_slot, unit, True)
                    copies.append(exchange(block_slot, unit, unit * slots + order))
                for unit in range(len(own_cuts)):
                    multiply(block_slot, unit, False)
                    with jax.named_scope(f"across_wait{unit}_{order}"):
                        copies[unit].wait_recv()
                    finish(block_slot, unit, order)

    second_block = pair + inner * (third - pair)
    third_block = third + inner * (fourth - third)
    fourth_block = fourth + inner * (pair - fourth)
    query_forwards = []

    def wait_queries(block_slot, only_outer=False):
        arrived = send_queries(block_slot, pair, 0)
        if only_outer:

            @pl.when(inner == 0)
            def _():
                with jax.named_scope("q_wait_outer"):
                    arrived.wait_recv()
        else:
            with jax.named_scope("q_wait_last"):
                arrived.wait_recv()

    def release_queries():
        @pl.when(inner == 1)
        def _():
            with jax.named_scope("second_q_sent"):
                second_queries.wait_send()
            pl.semaphore_signal(
                clear, inc=1, device_id={"seq": pair * per + place}, device_id_type=MESH
            )

        @pl.when(inner == 0)
        def _():
            with jax.named_scope("clear_wait"):
                pl.semaphore_wait(clear, 1)
            second_queries.start()

    with jax.named_scope("attend0"):
        attend(slot, release_queries)
    query_forwards.append(pass_on(third, 2))
    wait_queries(pair, only_outer=True)
    with jax.named_scope("attend1"):
        attend(second_block)
    own_weight.wait()
    own_products(second_block, 1)
    own_products(slot, 0)
    query_forwards.append(pass_on(fourth, 3))
    wait_queries(third, only_outer=True)
    with jax.named_scope("attend2"):
        attend(third_block)
    own_products(third_block, 2)
    wait_queries(fourth_block)
    with jax.named_scope("attend3"):
        attend(fourth_block)
    own_products(fourth_block, 3)

    for unit in range(len(own_cuts) if len(units) > 1 else 0, len(units)):
        _, _, sender, keeper = units[unit]
        with jax.named_scope(f"w_wait{unit}"):
            if sender is None:
                for copy in w_arrivals.values():
                    copy.wait_recv()
            else:
                w_arrivals[sender, cuts[(unit - len(own_cuts)) % len(cuts)][0]].wait_recv()
        index = len(own_cuts) * slots + unit

        def give():
            multiply(None, unit, True)
            exchange(None, unit, index)

        def keep():
            multiply(None, unit, False)
            with jax.named_scope(f"across_wait{unit}"):
                across_copy(unit, None, index, kept_part(unit)[2]).wait_recv()
            for order, block_slot in ((3, fourth), (2, third), (1, pair), (0, slot)):
                finish(block_slot, unit, order)

        if keeper is None:
            give()
            keep()
        else:
            pl.when(core == keeper)(keep)
            pl.when(core != keeper)(give)

    for source in range(tp_count):
        arrival = all_of(recv.at[source // 2, :, : out_width // 2], c_ss.at[0], c_rs.at[source])

        @pl.when(jnp.logical_or(g != source, g != slot))
        def _():
            with jax.named_scope(f"arrive{source}"):
                arrival.wait_recv()

    with jax.named_scope("send_waits"):
        all_segs.wait_send()
        all_of(q_ref.at[:, : 2 * (slots - 1) * HEAD_DIM], kv_ss, x_rs.at[0]).wait_send()
        for copy in started:
            copy.wait_send()
        for r in range(1, per):
            all_of(q_ref, x_ss.at[r - 1], x_rs.at[r - 1]).wait_send()
            all_of(w_all.at[:, :width], w_ss.at[r - 1], w_rs.at[0, 0]).wait_send()
        all_of(attended, d_ss, d_rs.at[0]).wait_send()
        all_of(attended.at[pl.ds(0, slots - 1)], c_ss.at[1], c_rs.at[0]).wait_send()

        @pl.when(g != slot)
        def _():
            all_of(attended.at[0], c_ss.at[0], c_rs.at[0]).wait_send()

        @pl.when(inner == 0)
        def _():
            second_queries.wait_send()

        @pl.when(inner == 1)
        def _():
            for copy in query_forwards:
                copy.wait_send()


def add_kernel(pieces, out_hbm, result, sems):
    bands = sems.shape[0]
    rows = result.shape[0] // bands
    copies = []
    for band in range(bands):
        where = slice(band * rows, (band + 1) * rows)
        total = pieces[0, where].astype(jnp.float32)
        for part in range(1, pieces.shape[0]):
            total = total + pieces[part, where].astype(jnp.float32)
        result[where] = total.astype(result.dtype)
        copy = pltpu.make_async_copy(result.at[where], out_hbm.at[where], sems.at[band])
        copy.start()
        copies.append(copy)
    for copy in copies:
        copy.wait()


def local(queries, keys, values, segment_ids, out_weight):
    rows = queries.shape[0]
    members = lax.axis_size("seq")
    slots = lax.axis_size("tp")
    per = members // slots
    heads = queries.shape[1] // HEAD_DIM
    out_width = out_weight.shape[1] * per
    width = out_weight.shape[1]
    if width % 1024 == 0:
        own_cuts = [(0, width // 2), (width // 2, width // 2)]
        cuts = [(0, width // 2), (width // 2, width // 4)]
        cuts += [(3 * width // 4, width // 8), (7 * width // 8, width // 8)]
        solo = 2 if per == 2 else 0
        units = len(own_cuts) + (per - 1) * len(cuts)
        half = width // 4
    else:
        own_cuts = cuts = [(0, width)]
        solo = 0
        units = 1
        half = out_width // 2
    chunk_count = 16
    tiles = members // 2
    group = heads
    while group > 1 and tiles * group * rows * 2 * rows * 4 > 20 * 1024 * 1024:
        group //= 2
    exponent = np.arange(HEAD_DIM // 2, dtype=np.float32) * np.float32(2.0 / HEAD_DIM)
    inverse = np.power(np.float32(rope_base), -exponent).astype(np.float32)
    inverse = jnp.asarray(np.concatenate([inverse, inverse])[None, :])
    vmem = pl.BlockSpec(memory_space=pltpu.VMEM)
    bf16, f32 = jnp.bfloat16, jnp.float32
    dma = pltpu.SemaphoreType.DMA
    buffers = [
        pltpu.VMEM((1, HEAD_DIM), f32),
        pltpu.VMEM(queries.shape, bf16),
        pltpu.VMEM(keys.shape, bf16),
        pltpu.VMEM((members, 1, rows), jnp.int32),
        pltpu.VMEM((tiles, 2 * rows, HEAD_DIM), bf16),
        pltpu.VMEM((tiles, 2 * rows, HEAD_DIM), bf16),
        pltpu.VMEM((slots, rows, queries.shape[1]), bf16),
        pltpu.VMEM((out_weight.shape[0], out_width), bf16),
        pltpu.VMEM((slots, rows, queries.shape[1]), bf16),
        pltpu.VMEM((group, rows, HEAD_DIM), f32),
        pltpu.VMEM((group, rows, HEAD_DIM), f32),
        pltpu.VMEM((group, rows, HEAD_DIM), f32),
        pltpu.VMEM((tiles, group, rows, 2 * rows), f32),
        pltpu.VMEM((slots, rows, HEAD_DIM), jnp.int32),
        pltpu.VMEM((units, slots, rows, half), bf16),
        pltpu.VMEM((units, slots, rows, half), bf16),
        pltpu.VMEM((slots, rows, half), f32),
        pltpu.VMEM((slots * units, rows, half), bf16),
    ]
    semaphores = [dma((5,))]
    semaphores += [dma(())] * 2
    semaphores += [dma(()), dma((slots,)), dma((slots - 1,))]
    semaphores += [dma((per - 1,))] * 2
    semaphores += [dma((slots,))] * 2
    semaphores += [dma((per - 1,)), dma((len(cuts), per - 1))]
    semaphores += [dma(()), pltpu.SemaphoreType.REGULAR]
    semaphores += [dma(()), dma((len(own_cuts) * slots + units,)), dma((2,))]
    semaphores += [dma((slots,))]
    on_chip = sum(math.prod(item.shape) * jnp.dtype(item.dtype).itemsize for item in buffers)
    operands = (inverse, queries, keys, values, segment_ids.reshape(1, rows), out_weight)
    pieces = pl.pallas_call(
        functools.partial(layer_kernel, members, slots, cuts, own_cuts, solo, chunk_count),
        out_shape=pltpu.VMEM((slots // 2, rows, out_width), bf16),
        in_specs=[pl.BlockSpec(memory_space=pl.ANY)] * 6,
        out_specs=pl.BlockSpec(memory_space=pltpu.VMEM),
        scratch_shapes=buffers + semaphores,
        compiler_params=pltpu.CompilerParams(
            collective_id=0, has_side_effects=True, vmem_limit_bytes=on_chip + 8 * 1024 * 1024
        ),
    )(*[pltpu.with_memory_space_constraint(x, pltpu.HBM) for x in operands])
    return pl.pallas_call(
        add_kernel,
        out_shape=jax.ShapeDtypeStruct((rows, out_width), bf16),
        in_specs=[vmem],
        out_specs=pl.BlockSpec(memory_space=pl.ANY),
        scratch_shapes=[pltpu.VMEM((rows, out_width), bf16), dma((4,))],
        compiler_params=pltpu.CompilerParams(vmem_limit_bytes=4 * 1024 * 1024),
    )(pieces)


def solution(mesh):
    return jax.shard_map(
        local,
        mesh=mesh,
        in_specs=(P("seq", "tp"), P("seq", "tp"), P("seq", "tp"), P("seq"), P("tp", "seq")),
        out_specs=P("seq", "tp"),
        check_vma=False,
    )
```
